8 devices in a mesh: dp: 1 (over z), ep: 8 (over y, x, core).
Axes of the slice: x: 2, y: 2, z: 1, core: 2. Of those that a mesh axis runs over, the one named last changes fastest.
Arguments:
- hidden: bfloat16 [8, 128, 2048], P(('dp', 'ep'))
- expert_ids: int32 [8, 128, 8], P(('dp', 'ep'))
- slot_ids: int32 [8, 128, 8], P(('dp', 'ep'))
- attn_norm: bfloat16 [2048], replicated
- w_query: bfloat16 [2048, 2048], replicated
- w_key: bfloat16 [2048, 2048], replicated
- w_value: bfloat16 [2048, 2048], replicated
- w_out: bfloat16 [16, 128, 2048], replicated
- ffn_norm: bfloat16 [2048], replicated
- ffn_gate: bfloat16 [2048, 8192], replicated
- ffn_up: bfloat16 [2048, 8192], replicated
- ffn_down: bfloat16 [8192, 2048], replicated
- moe_norm: bfloat16 [2048], replicated
- w_router: bfloat16 [2048, 64], replicated
- exp_gate: bfloat16 [64, 2048, 1024], P('ep')
- exp_up: bfloat16 [64, 2048, 1024], P('ep')
- exp_down: bfloat16 [64, 1024, 2048], P('ep')
Outputs:
- output: bfloat16 [8, 128, 2048], P(('dp', 'ep'))
All inputs are finite; a program needn't handle non-finite values.
Results may differ from the reference program's by a relative error of at most 0.00942246.
Values are sent between devices in bfloat16 or wider.
A program may use at most 1 GiB of HBM per device.

```python
import jax
import jax.numpy as jnp
from jax import lax

D_MODEL = 2048
N_HEADS = 16
KV_HEADS = 16
HEAD_DIM = 128
FF_DIM = 8192
N_EXPERTS = 64
TOP_K = 8
EXPERT_FF = 1024
SEQ_LEN = 128
BATCH_DEV = 1
GROUP_SIZE = 8

N_SEQS = GROUP_SIZE * BATCH_DEV
TOKENS_DEV = BATCH_DEV * SEQ_LEN
TOKENS = GROUP_SIZE * TOKENS_DEV
LOCAL_EXPERTS = N_EXPERTS // GROUP_SIZE
CAPACITY = 3 * TOKENS_DEV * TOP_K // N_EXPERTS
HOT_DEVICES = max(1, GROUP_SIZE // 8)
Q_PER_KV = N_HEADS // KV_HEADS
RMS_EPS = 1e-6
ROPE_BASE = 10000.0


def draw_routing(route_key):
    key_devs, key_rows = jax.random.split(route_key)
    mean_load = TOKENS_DEV * TOP_K // N_EXPERTS
    hot_count = HOT_DEVICES * LOCAL_EXPERTS
    cold_count = N_EXPERTS - hot_count
    cold_total = N_EXPERTS * mean_load - hot_count * CAPACITY
    cold_base = cold_total // cold_count
    cold_extra = cold_total - cold_base * cold_count
    expert_rank = jnp.arange(N_EXPERTS, dtype=jnp.int32)
    rank_load = jnp.where(expert_rank < hot_count, CAPACITY, cold_base + (expert_rank - hot_count < cold_extra).astype(jnp.int32))
    rank_start = jnp.cumsum(rank_load) - rank_load
    copy_rank = jnp.repeat(expert_rank, rank_load, total_repeat_length=TOKENS_DEV * TOP_K)
    copy_slot = jnp.arange(TOKENS_DEV * TOP_K, dtype=jnp.int32) - rank_start[copy_rank]
    dev_order = jax.random.permutation(key_devs, GROUP_SIZE)
    expert_of_rank = (dev_order[:, None] * LOCAL_EXPERTS + jnp.arange(LOCAL_EXPERTS)[None, :]).reshape(N_EXPERTS)
    base_ids = expert_of_rank[copy_rank].reshape(TOP_K, TOKENS_DEV).T
    base_slots = copy_slot.reshape(TOP_K, TOKENS_DEV).T

    def one_device(dev_key):
        key_perm, key_shift = jax.random.split(dev_key)
        row_order = jax.random.permutation(key_perm, TOKENS_DEV)
        col_shift = jax.random.randint(key_shift, (TOKENS_DEV, 1), 0, TOP_K)
        col_index = (jnp.arange(TOP_K)[None, :] + col_shift) % TOP_K
        dev_ids = jnp.take_along_axis(base_ids[row_order], col_index, axis=1)
        dev_slots = jnp.take_along_axis(base_slots[row_order], col_index, axis=1)
        return dev_ids, dev_slots

    dev_ids, dev_slots = jax.vmap(one_device)(jax.random.split(key_rows, GROUP_SIZE))
    return (dev_ids.astype(jnp.int32).reshape(N_SEQS, SEQ_LEN, TOP_K), dev_slots.astype(jnp.int32).reshape(N_SEQS, SEQ_LEN, TOP_K))


def draw_normal(draw_key, shape, std):
    return (jax.random.normal(draw_key, shape, jnp.float32) * std).astype(jnp.bfloat16)


def draw_gain(gain_key):
    return (1.0 + 0.4 * jax.random.normal(gain_key, (D_MODEL,), jnp.float32)).astype(jnp.bfloat16)


def setup_inputs(seed: int = 0, part: int = 0) -> dict:
    shared = jax.random.split(jax.random.key(seed), 14)
    part_key = jax.random.fold_in(jax.random.key(seed + 1), part)
    expert_ids, slot_ids = draw_routing(jax.random.fold_in(part_key, 3))
    q_width = N_HEADS * HEAD_DIM
    kv_width = KV_HEADS * HEAD_DIM
    return {
        'hidden': draw_normal(jax.random.fold_in(part_key, 1), (N_SEQS, SEQ_LEN, D_MODEL), 1.0),
        'expert_ids': expert_ids,
        'slot_ids': slot_ids,
        'attn_norm': draw_gain(shared[0]),
        'w_query': draw_normal(shared[1], (D_MODEL, q_width), 2.0 * D_MODEL ** -0.5),
        'w_key': draw_normal(shared[2], (D_MODEL, kv_width), D_MODEL ** -0.5),
        'w_value': draw_normal(shared[3], (D_MODEL, kv_width), D_MODEL ** -0.5),
        'w_out': draw_normal(shared[4], (N_HEADS, HEAD_DIM, D_MODEL), 2.0 * q_width ** -0.5),
        'ffn_norm': draw_gain(shared[5]),
        'ffn_gate': draw_normal(shared[6], (D_MODEL, FF_DIM), D_MODEL ** -0.5),
        'ffn_up': draw_normal(shared[7], (D_MODEL, FF_DIM), D_MODEL ** -0.5),
        'ffn_down': draw_normal(shared[8], (FF_DIM, D_MODEL), FF_DIM ** -0.5),
        'moe_norm': draw_gain(shared[9]),
        'w_router': draw_normal(shared[10], (D_MODEL, N_EXPERTS), 1.5 * D_MODEL ** -0.5),
        'exp_gate': draw_normal(shared[11], (N_EXPERTS, D_MODEL, EXPERT_FF), D_MODEL ** -0.5),
        'exp_up': draw_normal(shared[12], (N_EXPERTS, D_MODEL, EXPERT_FF), D_MODEL ** -0.5),
        'exp_down': draw_normal(shared[13], (N_EXPERTS, EXPERT_FF, D_MODEL), 2.0 * EXPERT_FF ** -0.5),
    }


def rms_norm(row_vals, norm_scale):
    as_float = row_vals.astype(jnp.float32)
    inv_rms = lax.rsqrt(jnp.mean(as_float * as_float, axis=-1, keepdims=True) + RMS_EPS)
    return (as_float * inv_rms * norm_scale.astype(jnp.float32)).astype(jnp.bfloat16)


def rotary(head_vals):
    half_dim = HEAD_DIM // 2
    inv_freq = ROPE_BASE ** (-2.0 * jnp.arange(half_dim, dtype=jnp.float32) / HEAD_DIM)
    angles = jnp.arange(SEQ_LEN, dtype=jnp.float32)[:, None] * inv_freq[None, :]
    cos_t = jnp.cos(angles)[:, None, :]
    sin_t = jnp.sin(angles)[:, None, :]
    first_half = head_vals[..., :half_dim]
    second_half = head_vals[..., half_dim:]
    return jnp.concatenate([first_half * cos_t - second_half * sin_t, second_half * cos_t + first_half * sin_t], axis=-1)


def reference(hidden, expert_ids, slot_ids, attn_norm, w_query, w_key, w_value, w_out, ffn_norm, ffn_gate, ffn_up, ffn_down, moe_norm, w_router, exp_gate, exp_up, exp_down):
    causal = jnp.arange(SEQ_LEN)[:, None] >= jnp.arange(SEQ_LEN)[None, :]
    out_mat = w_out.reshape(N_HEADS * HEAD_DIM, D_MODEL)

    def dense_seq(seq_rows):
        normed = rms_norm(seq_rows, attn_norm)
        queries = rotary(jnp.dot(normed, w_query, preferred_element_type=jnp.float32).reshape(SEQ_LEN, N_HEADS, HEAD_DIM)).astype(jnp.bfloat16)
        key_vals = rotary(jnp.dot(normed, w_key, preferred_element_type=jnp.float32).reshape(SEQ_LEN, KV_HEADS, HEAD_DIM)).astype(jnp.bfloat16)
        values = jnp.dot(normed, w_value, preferred_element_type=jnp.float32).astype(jnp.bfloat16).reshape(SEQ_LEN, KV_HEADS, HEAD_DIM)
        grouped = queries.reshape(SEQ_LEN, KV_HEADS, Q_PER_KV, HEAD_DIM)
        scores = jnp.einsum('sgrd,tgd->grst', grouped.astype(jnp.float32), key_vals.astype(jnp.float32)) * HEAD_DIM ** -0.5
        scores = jnp.where(causal, scores, -jnp.inf)
        attn_prob = jax.nn.softmax(scores, axis=-1).astype(jnp.bfloat16)
        context = jnp.einsum('grst,tgd->sgrd', attn_prob.astype(jnp.float32), values.astype(jnp.float32)).astype(jnp.bfloat16)
        attn_out = (seq_rows.astype(jnp.float32) + jnp.dot(context.reshape(SEQ_LEN, N_HEADS * HEAD_DIM), out_mat, preferred_element_type=jnp.float32)).astype(jnp.bfloat16)
        normed_ffn = rms_norm(attn_out, ffn_norm)
        hidden_act = (jax.nn.silu(jnp.dot(normed_ffn, ffn_gate, preferred_element_type=jnp.float32)) * jnp.dot(normed_ffn, ffn_up, preferred_element_type=jnp.float32)).astype(jnp.bfloat16)
        return attn_out.astype(jnp.float32) + jnp.dot(hidden_act, ffn_down, preferred_element_type=jnp.float32)

    dense_out = lax.map(dense_seq, hidden).reshape(TOKENS, D_MODEL)

    token_rows = hidden.reshape(TOKENS, D_MODEL)
    choice_ids = expert_ids.reshape(TOKENS, TOP_K)
    choice_slots = slot_ids.reshape(TOKENS, TOP_K)
    normed = rms_norm(token_rows, moe_norm)
    logits = jnp.dot(normed, w_router, preferred_element_type=jnp.float32)
    gate_vals = jax.nn.softmax(jnp.take_along_axis(logits, choice_ids, axis=1), axis=-1)
    src_dev = jnp.arange(TOKENS, dtype=jnp.int32) // TOKENS_DEV
    buf_pos = (choice_ids * GROUP_SIZE + src_dev[:, None]) * CAPACITY + choice_slots
    buf_rows = N_EXPERTS * GROUP_SIZE * CAPACITY
    owner_copy = jnp.full((buf_rows,), TOKENS * TOP_K, jnp.int32).at[buf_pos.reshape(-1)].set(jnp.arange(TOKENS * TOP_K, dtype=jnp.int32))
    padded = jnp.concatenate([normed, jnp.zeros((1, D_MODEL), jnp.bfloat16)], axis=0)
    gate_ext = jnp.concatenate([gate_vals.reshape(-1), jnp.zeros((1,), jnp.float32)])

    def one_expert(moe_acc, operands):
        copy_index, gate_w, up_w, down_w = operands
        token_index = copy_index // TOP_K
        expert_rows = padded[token_index]
        z_gate = jnp.dot(expert_rows, gate_w, preferred_element_type=jnp.float32)
        z_up = jnp.dot(expert_rows, up_w, preferred_element_type=jnp.float32)
        hidden_act = (jax.nn.silu(z_gate) * z_up).astype(jnp.bfloat16)
        expert_y = jnp.dot(hidden_act, down_w, preferred_element_type=jnp.float32).astype(jnp.bfloat16)
        weighted = gate_ext[copy_index][:, None] * expert_y.astype(jnp.float32)
        return moe_acc.at[token_index].add(weighted), None

    moe_acc = lax.scan(one_expert, jnp.zeros((TOKENS + 1, D_MODEL), jnp.float32), (owner_copy.reshape(N_EXPERTS, GROUP_SIZE * CAPACITY), exp_gate, exp_up, exp_down))[0]
    moe_out = moe_acc[:TOKENS]
    return (dense_out + moe_out).astype(jnp.bfloat16).reshape(N_SEQS, SEQ_LEN, D_MODEL)
```

```python
import functools

import jax
import jax.numpy as jnp
import numpy as np
from jax import lax
from jax.experimental import pallas as pl
from jax.experimental.pallas import tpu as pltpu
from jax.sharding import PartitionSpec as P

RMS_EPS = 1e-6
ROPE_BASE = 10000.0
F32 = jnp.float32
BF16 = jnp.bfloat16

DEVS = 8
TOK = 128
DM = 2048
HEAD = 128
FF = 8192
LOCAL = 8
EFF = 1024
TOPK = 8
CAP = 48
ROWS = LOCAL * CAP
NEXP = DEVS * LOCAL
CW = 512
NCB = DM // CW
NSLOT = 8
FF_EARLY = 6

N_QKV = 12
N_OUT = 4
N_FFA = 2 * FF_EARLY
N_EGU = 4 * LOCAL
N_EDN = NCB * (LOCAL // 2)
N_FFB = 2 * (FF // CW - FF_EARLY)
N_FDN = NCB * (FF // DM)
G_QKV = 0
G_OUT = G_QKV + N_QKV
G_FFA = G_OUT + N_OUT
G_EGU = G_FFA + N_FFA
G_EDN = G_EGU + N_EGU
G_FFB = G_EDN + N_EDN
G_FDN = G_FFB + N_FFB
G_END = G_FDN + N_FDN


def aligned(index, size):
    return pl.ds(pl.multiple_of(index * size, size), size)


def dot(lhs, rhs):
    return jnp.dot(lhs, rhs, preferred_element_type=F32)


def rms(as_float, scale):
    inv_rms = lax.rsqrt(jnp.mean(as_float * as_float, axis=-1, keepdims=True) + RMS_EPS)
    return (as_float * inv_rms * scale.astype(F32)).astype(BF16)


def silu_mul(z_gate, z_up):
    return (jax.nn.silu(z_gate) * z_up).astype(BF16)


def kernel(hid, ids, slots, attn_norm, ffn_norm, moe_norm, w_router, cos_t, sin_t,
           w_query, w_key, w_value, w_out, ffn_gate, ffn_up, ffn_down, exp_gate, exp_up, exp_down,
           out,
           ring, toks, disp, hexp, pown, psib, recv0, recv1, gates, route, pay, ctx, xn, a_s, hff, facc, qs, ks, vs,
           ring_sem, ag_send, ag_recv, rt_send, rt_recv, s0_send, s0_recv, s1_send, s1_recv):
    me = lax.axis_index("ep")
    chip = me // 2
    core = me % 2
    sib = chip * 2 + 1 - core
    rel_chips = (chip + 1 - 2 * (chip % 2), (chip + 2) % 4, 3 - chip)

    def start(g, slot):
        def fetch(src, rows=None):
            dst = ring.at[slot] if rows is None else ring.at[slot, rows]
            pltpu.make_async_copy(src, dst, ring_sem.at[slot]).start()

        def within(lo, hi):
            return pl.when(jnp.logical_and(g >= lo, g < hi))

        @within(G_QKV, G_OUT)
        def _():
            col, kind = g // 3, g % 3
            for which, mat in enumerate((w_query, w_key, w_value)):
                @pl.when(kind == which)
                def _():
                    fetch(mat.at[:, aligned(col, CW)])

        @within(G_OUT, G_FFA)
        def _():
            fetch(w_out.at[:, aligned(g - G_OUT, CW)])

        def ff_pair(local, first):
            col, kind = first + local // 2, local % 2

            @pl.when(kind == 0)
            def _():
                fetch(ffn_gate.at[:, aligned(col, CW)])

            @pl.when(kind == 1)
            def _():
                fetch(ffn_up.at[:, aligned(col, CW)])

        @within(G_FFA, G_EGU)
        def _():
            ff_pair(g - G_FFA, 0)

        @within(G_EGU, G_EDN)
        def _():
            local = g - G_EGU
            expert, col, kind = local // 4, (local // 2) % 2, local % 2

            @pl.when(kind == 0)
            def _():
                fetch(exp_gate.at[expert, :, aligned(col, CW)])

            @pl.when(kind == 1)
            def _():
                fetch(exp_up.at[expert, :, aligned(col, CW)])

        @within(G_EDN, G_FFB)
        def _():
            local = g - G_EDN
            col, pair = local // 4, local % 4
            for i in range(2):
                fetch(exp_down.at[pair * 2 + i, :, aligned(col, CW)], pl.ds(i * EFF, EFF))

        @within(G_FFB, G_FDN)
        def _():
            ff_pair(g - G_FFB, FF_EARLY)

        @within(G_FDN, G_END)
        def _():
            local = g - G_FDN
            fetch(ffn_down.at[aligned(local % 4, DM), aligned(local // 4, CW)])

    def ready(g):
        slot = g % NSLOT
        pltpu.make_async_copy(w_query.at[:, pl.ds(0, CW)], ring.at[slot], ring_sem.at[slot]).wait()
        return slot

    def done(g):
        start(g + NSLOT, g % NSLOT)

    def ag_copy(src, peer, index):
        return pltpu.make_async_remote_copy(toks.at[src], toks.at[src], ag_send.at[index], ag_recv.at[src], device_id={"ep": peer}, device_id_type=pl.DeviceIdType.MESH)

    def rt_copy(src, peer, index):
        return pltpu.make_async_remote_copy(route.at[src], route.at[src], rt_send.at[index], rt_recv.at[src], device_id={"ep": peer}, device_id_type=pl.DeviceIdType.MESH)

    def s0_copy(b):
        return pltpu.make_async_remote_copy(psib.at[b % 2], recv0.at[b], s0_send.at[b % 2], s0_recv.at[b], device_id={"ep": sib}, device_id_type=pl.DeviceIdType.MESH)

    def s1_copy(b, rel):
        return pltpu.make_async_remote_copy(pown.at[b, rel_chips[rel]], recv1.at[b, rel], s1_send.at[b, rel], s1_recv.at[b, rel], device_id={"ep": rel_chips[rel] * 2 + core}, device_id_type=pl.DeviceIdType.MESH)

    peers = tuple(c * 2 + core for c in rel_chips) + (sib,)

    for g in range(NSLOT):
        start(jnp.int32(g), g)
    barrier = pltpu.get_barrier_semaphore()
    for peer in peers:
        pl.semaphore_signal(barrier, inc=1, device_id={"ep": peer}, device_id_type=pl.DeviceIdType.MESH)

    hid_f = hid[...].astype(F32)
    inv_rms = lax.rsqrt(jnp.mean(hid_f * hid_f, axis=-1, keepdims=True) + RMS_EPS)
    for cb in range(NCB):
        part = hid[:, cb * CW:(cb + 1) * CW].astype(F32) * inv_rms
        toks[me, cb * TOK:(cb + 1) * TOK, :] = (part * moe_norm[:, cb * CW:(cb + 1) * CW].astype(F32)).astype(BF16)
        xn[:, cb * CW:(cb + 1) * CW] = (part * attn_norm[:, cb * CW:(cb + 1) * CW].astype(F32)).astype(BF16)

    logits = jnp.zeros((TOK, NEXP), F32)
    for cb in range(NCB):
        logits = logits + dot(toks[me, cb * TOK:(cb + 1) * TOK, :], w_router[cb * CW:(cb + 1) * CW, :])
    expert_iota = lax.broadcasted_iota(jnp.int32, (TOK, NEXP), 1)
    chosen = [jnp.sum(jnp.where(expert_iota == ids[:, j:j + 1], logits, 0.0), axis=-1, keepdims=True) for j in range(TOPK)]
    top = functools.reduce(jnp.maximum, chosen)
    raised = [jnp.exp(c - top) for c in chosen]
    total = functools.reduce(jnp.add, raised)
    pay[...] = jnp.zeros_like(pay)
    pay[:, 0:TOPK] = (ids[...] * CAP + slots[...]).astype(F32)
    for j in range(TOPK):
        pay[:, TOPK + j:TOPK + j + 1] = raised[j] / total
    route[me] = jnp.transpose(pay[...])[0:2 * TOPK, :]

    pl.semaphore_wait(barrier, 4)
    for index, peer in enumerate(peers):
        ag_copy(me, peer, index).start()

    row_i = lax.broadcasted_iota(jnp.int32, (TOK, TOK), 0)
    col_i = lax.broadcasted_iota(jnp.int32, (TOK, TOK), 1)
    causal = row_i >= col_i

    def rope_into(dst, vals):
        for h in range(CW // HEAD):
            part = vals[:, h * HEAD:(h + 1) * HEAD]
            turned = part * cos_t[...] + pltpu.roll(part, HEAD // 2, 1) * sin_t[...]
            dst[:, h * HEAD:(h + 1) * HEAD] = turned.astype(BF16)

    def attn_group(hg, carry):
        g = G_QKV + hg * 3
        slot = ready(g)
        rope_into(qs, dot(xn[...], ring[slot]))
        done(g)

        @pl.when(hg == 0)
        def _():
            for index, peer in enumerate(peers):
                rt_copy(me, peer, index).start()

        slot = ready(g + 1)
        rope_into(ks, dot(xn[...], ring[slot]))
        done(g + 1)
        slot = ready(g + 2)
        vs[...] = dot(xn[...], ring[slot]).astype(BF16)
        done(g + 2)
        for h in range(CW // HEAD):
            cols = slice(h * HEAD, (h + 1) * HEAD)
            scores = lax.dot_general(qs[:, cols], ks[:, cols], (((1,), (1,)), ((), ())), preferred_element_type=F32) * HEAD ** -0.5
            scores = jnp.where(causal, scores, -jnp.inf)
            expd = jnp.exp(scores - jnp.max(scores, axis=-1, keepdims=True))
            prob = (expd / jnp.sum(expd, axis=-1, keepdims=True)).astype(BF16)
            ctx[:, pl.ds(pl.multiple_of(hg * CW + h * HEAD, HEAD), HEAD)] = dot(prob, vs[:, cols]).astype(BF16)
        return carry

    lax.fori_loop(0, NCB, attn_group, 0)

    def out_block(n, carry):
        g = G_OUT + n
        slot = ready(g)
        cols = aligned(n, CW)
        a_s[:, cols] = (hid[:, cols].astype(F32) + dot(ctx[...], ring[slot])).astype(BF16)
        done(g)
        return carry

    lax.fori_loop(0, N_OUT, out_block, 0)
    xn[...] = rms(a_s[...].astype(F32), ffn_norm[...])

    def forward(rel):
        src = rel_chips[rel] * 2 + core
        ag_copy(src, sib, 4 + rel).wait_recv()
        ag_copy(src, sib, 4 + rel).start()
        rt_copy(src, sib, 4 + rel).wait_recv()
        rt_copy(src, sib, 4 + rel).start()

    forward(0)
    forward(1)

    def ffn_pair(g, col):
        slot = ready(g)
        z_gate = dot(xn[...], ring[slot])
        done(g)
        slot = ready(g + 1)
        z_up = dot(xn[...], ring[slot])
        done(g + 1)
        hff[:, aligned(col, CW)] = silu_mul(z_gate, z_up)

    def ffn_early(i, carry):
        ffn_pair(G_FFA + 2 * i, i)
        return carry

    lax.fori_loop(0, FF_EARLY, ffn_early, 0)

    forward(2)
    ag_copy(sib, sib, 0).wait_recv()
    rt_copy(sib, sib, 0).wait_recv()
    for rel in range(3):
        src = rel_chips[rel] * 2 + 1 - core
        ag_copy(src, sib, 0).wait_recv()
        rt_copy(src, sib, 0).wait_recv()

    def dispatch(src, carry):
        want = lax.broadcasted_iota(jnp.int32, (ROWS, TOK), 0).astype(F32) + (me * ROWS).astype(F32)
        pick = jnp.zeros((ROWS, TOK), F32)
        gate = jnp.zeros((ROWS, TOK), F32)
        for j in range(TOPK):
            hit = route[src, j:j + 1, :] == want
            pick = jnp.where(hit, 1.0, pick)
            gate = jnp.where(hit, route[src, TOPK + j:TOPK + j + 1, :], gate)
        gate_t = jnp.transpose(gate)
        high = gate_t.astype(BF16)
        rest = gate_t - high.astype(F32)
        mid = rest.astype(BF16)
        low = (rest - mid.astype(F32)).astype(BF16)
        gates[src, 0:TOK, :] = high
        gates[src, TOK:2 * TOK, :] = mid
        gates[src, 2 * TOK:3 * TOK, :] = low
        pick = pick.astype(BF16)
        for cb in range(NCB):
            rows = dot(pick, toks[src, cb * TOK:(cb + 1) * TOK, :]).astype(BF16)
            for e in range(LOCAL):
                disp[e, pl.ds(pl.multiple_of(src * CAP, 16), CAP), cb * CW:(cb + 1) * CW] = rows[e * CAP:(e + 1) * CAP, :]
        return carry

    lax.fori_loop(0, DEVS, dispatch, 0)

    for index, peer in enumerate(peers):
        ag_copy(me, peer, index).wait_send()
        rt_copy(me, peer, index).wait_send()
    for rel in range(3):
        src = rel_chips[rel] * 2 + core
        ag_copy(src, sib, 4 + rel).wait_send()
        rt_copy(src, sib, 4 + rel).wait_send()

    def expert_up(i, carry):
        g = G_EGU + 2 * i
        expert, col = i // 2, i % 2
        slot = ready(g)
        slot_up = ready(g + 1)
        for half in range(2):
            cols = slice(half * 256, (half + 1) * 256)
            z_gate = dot(disp[expert], ring[slot, :, cols])
            z_up = dot(disp[expert], ring[slot_up, :, cols])
            hexp[expert, :, pl.ds(pl.multiple_of(col * CW + half * 256, 256), 256)] = silu_mul(z_gate, z_up)
        done(g)
        done(g + 1)
        return carry

    lax.fori_loop(0, 2 * LOCAL, expert_up, 0)

    def fold(b):
        s0_copy(b).wait_recv()
        for c in range(4):
            pown[b, c] = pown[b, c] + recv0[b, c]

    def send1(b):
        for rel in range(3):
            s1_copy(b, rel).start()

    def down_block(b, carry):
        def down_pair(pair, inner):
            g = G_EDN + b * 4 + pair
            slot = ready(g)
            for i in range(2):
                e = pair * 2 + i
                y = dot(hexp[e], ring[slot, i * EFF:(i + 1) * EFF, :]).astype(BF16)
                for s in range(DEVS):
                    toks[s, pl.ds(pl.multiple_of(e * CAP, 16), CAP), :] = y[s * CAP:(s + 1) * CAP, :]
            done(g)

            @pl.when(jnp.logical_and(b >= 1, pair == 0))
            def _():
                s0_copy(b - 1).start()

            @pl.when(jnp.logical_and(b >= 1, pair == 2))
            def _():
                fold(b - 1)

            @pl.when(jnp.logical_and(b >= 1, pair == 3))
            def _():
                send1(b - 1)
            return inner

        lax.fori_loop(0, LOCAL // 2, down_pair, 0)

        @pl.when(b >= 2)
        def _():
            s0_copy(b - 2).wait_send()

        def combine(s):
            parts = dot(gates[s], toks[s, 0:ROWS, :])
            return parts[0:TOK] + parts[TOK:2 * TOK] + parts[2 * TOK:3 * TOK]

        def per_chip(c, inner):
            pown[b, c] = combine(c * 2 + core)
            psib[b % 2, c] = combine(c * 2 + 1 - core)
            return inner

        lax.fori_loop(0, 4, per_chip, 0)
        return carry

    lax.fori_loop(0, NCB, down_block, 0)

    def ffn_late(i, carry):
        ffn_pair(G_FFB + 2 * i, FF_EARLY + i)

        @pl.when(i == 0)
        def _():
            s0_copy(NCB - 1).start()

        @pl.when(i == 2)
        def _():
            fold(NCB - 1)

        @pl.when(i == 3)
        def _():
            send1(NCB - 1)
        return carry

    lax.fori_loop(0, FF // CW - FF_EARLY, ffn_late, 0)

    def down_out(n, carry):
        cols = aligned(n, CW)
        for kk in range(FF // DM):
            g = G_FDN + n * 4 + kk
            slot = ready(g)
            part = dot(hff[:, kk * DM:(kk + 1) * DM], ring[slot])
            if kk == 0:
                facc[...] = part
            else:
                facc[...] = facc[...] + part

            @pl.when(g + NSLOT < G_END)
            def _():
                done(g)
        for rel in range(3):
            s1_copy(n, rel).wait_recv()
        moe = pown[n, chip] + recv1[n, 0] + recv1[n, 1] + recv1[n, 2]
        out[:, cols] = (a_s[:, cols].astype(F32) + facc[...] + moe).astype(BF16)
        return carry

    lax.fori_loop(0, NCB, down_out, 0)

    for b in (NCB - 2, NCB - 1):
        s0_copy(b).wait_send()
    for b in range(NCB):
        for rel in range(3):
            s1_copy(b, rel).wait_send()


def rope_tables():
    half = HEAD // 2
    inv_freq = np.float32(ROPE_BASE) ** (np.float32(-2.0) * np.arange(half, dtype=np.float32) / np.float32(HEAD))
    angles = np.arange(TOK, dtype=np.float32)[:, None] * inv_freq[None, :].astype(np.float32)
    cos_h, sin_h = np.cos(angles).astype(np.float32), np.sin(angles).astype(np.float32)
    return np.concatenate([cos_h, cos_h], axis=1), np.concatenate([-sin_h, sin_h], axis=1)


def solution(mesh):
    row_spec = P(('dp', 'ep'), None, None)
    vec_spec = P(None)
    mat_spec = P(None, None)
    cube_spec = P(None, None, None)
    expert_spec = P('ep', None, None)
    vmem = pl.BlockSpec(memory_space=pltpu.VMEM)
    hbm = pl.BlockSpec(memory_space=pl.ANY)

    def per_device(hidden, expert_ids, slot_ids, attn_norm, w_query, w_key, w_value, w_out, ffn_norm, ffn_gate, ffn_up, ffn_down, moe_norm, w_router, exp_gate, exp_up, exp_down):
        cos_t, sin_t = rope_tables()
        dma = pltpu.SemaphoreType.DMA
        call = pl.pallas_call(
            kernel,
            out_shape=jax.ShapeDtypeStruct((TOK, DM), BF16),
            in_specs=[vmem] * 9 + [hbm] * 10,
            out_specs=vmem,
            scratch_shapes=[
                pltpu.VMEM((NSLOT, DM, CW), BF16),
                pltpu.VMEM((DEVS, NCB * TOK, CW), BF16),
                pltpu.VMEM((LOCAL, DEVS * CAP, DM), BF16),
                pltpu.VMEM((LOCAL, DEVS * CAP, EFF), BF16),
                pltpu.VMEM((NCB, 4, TOK, CW), F32),
                pltpu.VMEM((2, 4, TOK, CW), F32),
                pltpu.VMEM((NCB, 4, TOK, CW), F32),
                pltpu.VMEM((NCB, 3, TOK, CW), F32),
                pltpu.VMEM((DEVS, 3 * TOK, ROWS), BF16),
                pltpu.VMEM((DEVS, 2 * TOPK, TOK), F32),
                pltpu.VMEM((TOK, TOK), F32),
                pltpu.VMEM((TOK, DM), BF16),
                pltpu.VMEM((TOK, DM), BF16),
                pltpu.VMEM((TOK, DM), BF16),
                pltpu.VMEM((TOK, FF), BF16),
                pltpu.VMEM((TOK, CW), F32),
                pltpu.VMEM((TOK, CW), BF16),
                pltpu.VMEM((TOK, CW), BF16),
                pltpu.VMEM((TOK, CW), BF16),
                dma((NSLOT,)), dma((7,)), dma((DEVS,)), dma((7,)), dma((DEVS,)),
                dma((2,)), dma((NCB,)), dma((NCB, 3)), dma((NCB, 3)),
            ],
            compiler_params=pltpu.CompilerParams(collective_id=0, has_side_effects=True, vmem_limit_bytes=67043328),
            cost_estimate=pl.CostEstimate(flops=56_000_000_000, bytes_accessed=240_000_000, transcendentals=0),
        )
        res = call(
            hidden.reshape(TOK, DM), expert_ids.reshape(TOK, TOPK), slot_ids.reshape(TOK, TOPK),
            attn_norm.reshape(1, DM), ffn_norm.reshape(1, DM), moe_norm.reshape(1, DM), w_router, cos_t, sin_t,
            w_query, w_key, w_value, w_out.reshape(DM, DM), ffn_gate, ffn_up, ffn_down, exp_gate, exp_up, exp_down)
        return res.reshape(hidden.shape)

    return jax.shard_map(per_device, mesh=mesh, in_specs=(row_spec, row_spec, row_spec, vec_spec, mat_spec, mat_spec, mat_spec, cube_spec, vec_spec, mat_spec, mat_spec, mat_spec, vec_spec, mat_spec, expert_spec, expert_spec, expert_spec), out_specs=row_spec, check_vma=False)
```

```python
import functools

import jax
import jax.numpy as jnp
import numpy as np
from jax import lax
from jax.experimental import pallas as pl
from jax.experimental.pallas import tpu as pltpu
from jax.sharding import PartitionSpec as P

RMS_EPS = 1e-6
ROPE_BASE = 10000.0
F32 = jnp.float32
BF16 = jnp.bfloat16

DEVS = 8
TOK = 128
HALF = TOK // 2
DM = 2048
HEAD = 128
FF = 8192
LOCAL = 8
EFF = 1024
TOPK = 8
LANE = 128
CAP = 48
ROWS = LOCAL * CAP
NEXP = DEVS * LOCAL
CW = 512
NCB = DM // CW
NSLOT = 8
FF_EARLY = 5

N_QKV = 12
N_OUT = 4
N_FFA = 2 * FF_EARLY
N_EGU = 4 * LOCAL
N_EDN = NCB * (LOCAL // 2)
N_LATE = FF // CW - FF_EARLY
N_FFB = 2 * N_LATE
N_FDN = NCB * (FF // DM)
G_QKV = 0
G_OUT = G_QKV + N_QKV
G_FFA = G_OUT + N_OUT
G_EGU = G_FFA + N_FFA
G_EDN = G_EGU + N_EGU
G_FFB = G_EDN + N_EDN
G_FDN = G_FFB + N_FFB
G_END = G_FDN + N_FDN


def aligned(index, size):
    return pl.ds(pl.multiple_of(index * size, size), size)


def dot(lhs, rhs):
    return jnp.dot(lhs, rhs, preferred_element_type=F32)


def silu_mul(z_gate, z_up):
    return (jax.nn.silu(z_gate) * z_up).astype(BF16)


def kernel(hid, ids, slots, attn_norm, ffn_norm, moe_norm, w_router, cos_t, sin_t,
           w_query, w_key, w_value, w_out, ffn_gate, ffn_up, ffn_down, exp_gate, exp_up, exp_down,
           out,
           ring, toks, disp, hexp, pown, psib, recv0, recv1, recv2, gates, route, ctx, xn, a_s, hff, facc, qs, ks, vs, obuf,
           ring_sem, ag_send, ag_recv, rt_send, rt_recv, s0_send, s0_recv, s1_send, s1_recv, s2_send, s2_recv, out_sem):
    me = lax.axis_index("ep")
    chip = me // 2
    core = me % 2
    sib = chip * 2 + 1 - core
    chip_x, chip_y, chip_d = chip + 1 - 2 * (chip % 2), (chip + 2) % 4, 3 - chip
    src_x, src_y, src_d = chip_x * 2 + core, chip_y * 2 + core, chip_d * 2 + core

    def start(g, slot):
        def fetch(src, rows=None):
            dst = ring.at[slot] if rows is None else ring.at[slot, rows]
            pltpu.make_async_copy(src, dst, ring_sem.at[slot]).start()

        def within(lo, hi):
            return pl.when(jnp.logical_and(g >= lo, g < hi))

        @within(G_QKV, G_OUT)
        def _():
            col, kind = g // 3, g % 3
            for which, mat in enumerate((w_query, w_key, w_value)):
                @pl.when(kind == which)
                def _():
                    fetch(mat.at[:, aligned(col, CW)])

        @within(G_OUT, G_FFA)
        def _():
            fetch(w_out.at[:, aligned(g - G_OUT, CW)])

        def ff_pair(local, first):
            col, kind = first + local // 2, local % 2

            @pl.when(kind == 0)
            def _():
                fetch(ffn_gate.at[:, aligned(col, CW)])

            @pl.when(kind == 1)
            def _():
                fetch(ffn_up.at[:, aligned(col, CW)])

        @within(G_FFA, G_EGU)
        def _():
            ff_pair(g - G_FFA, 0)

        @within(G_EGU, G_EDN)
        def _():
            local = g - G_EGU
            expert, col, kind = local // 4, (local // 2) % 2, local % 2

            @pl.when(kind == 0)
            def _():
                fetch(exp_gate.at[expert, :, aligned(col, CW)])

            @pl.when(kind == 1)
            def _():
                fetch(exp_up.at[expert, :, aligned(col, CW)])

        @within(G_EDN, G_FFB)
        def _():
            local = g - G_EDN
            col, pair = local // 4, local % 4
            for i in range(2):
                fetch(exp_down.at[pair * 2 + i, :, aligned(col, CW)], pl.ds(i * EFF, EFF))

        @within(G_FFB, G_FDN)
        def _():
            ff_pair(g - G_FFB, FF_EARLY)

        @within(G_FDN, G_END)
        def _():
            local = g - G_FDN
            fetch(ffn_down.at[aligned(local % 4, DM), aligned(local // 4, CW)])

    def ready(g):
        slot = g % NSLOT
        pltpu.make_async_copy(w_query.at[:, pl.ds(0, CW)], ring.at[slot], ring_sem.at[slot]).wait()
        return slot

    def done(g):
        start(g + NSLOT, g % NSLOT)

    def send(src, dst, send_sem, recv_sem, peer):
        return pltpu.make_async_remote_copy(src, dst, send_sem, recv_sem, device_id={"ep": peer}, device_id_type=pl.DeviceIdType.MESH)

    def ag_copy(src, cb, link):
        block = toks.at[src, pl.ds(cb * TOK, TOK)]
        return send(block, block, ag_send.at[link, src, cb], ag_recv.at[src, cb], (src_x, src_y, sib)[link])

    def rt_copy(src, step):
        return send(route.at[src], route.at[src], rt_send.at[step], rt_recv.at[src], (me + step) % DEVS)

    def s0_copy(b, c):
        return send(psib.at[b % 2, c], recv0.at[b, c], s0_send.at[b % 2, c], s0_recv.at[b, c], sib)

    first_chip, first_dev = (chip_x, chip_y), (src_x, src_y)
    second_chip, second_dev = (chip_y, chip_x), (src_y, src_x)

    def s1_copy(b, half, which):
        dest = first_chip[half] if which == 0 else chip_d
        return send(pown.at[b, dest, pl.ds(half * HALF, HALF)], recv1.at[b, half, which], s1_send.at[b, half, which], s1_recv.at[b, half, which], first_dev[half])

    def s2_copy(b, half):
        return send(pown.at[b, second_chip[half], pl.ds(half * HALF, HALF)], recv2.at[b, half], s2_send.at[b, half], s2_recv.at[b, half], second_dev[half])

    for g in range(NSLOT):
        start(jnp.int32(g), g)
    barrier = pltpu.get_barrier_semaphore()
    for step in range(1, DEVS):
        pl.semaphore_signal(barrier, inc=1, device_id={"ep": (me + step) % DEVS}, device_id_type=pl.DeviceIdType.MESH)

    hid_f = hid[...].astype(F32)
    inv_rms = lax.rsqrt(jnp.mean(hid_f * hid_f, axis=-1, keepdims=True) + RMS_EPS)
    for lt in range(DM // LANE):
        cols = slice(lt * LANE, (lt + 1) * LANE)
        cb, within_cb = divmod(lt * LANE, CW)
        part = hid[:, cols].astype(F32) * inv_rms
        toks[me, cb * TOK:(cb + 1) * TOK, within_cb:within_cb + LANE] = (part * moe_norm[lt:lt + 1, :].astype(F32)).astype(BF16)
        xn[:, cols] = (part * attn_norm[lt:lt + 1, :].astype(F32)).astype(BF16)

    logits = jnp.zeros((NEXP, TOK), F32)
    for cb in range(NCB):
        logits = logits + lax.dot_general(w_router[:, cb * CW:(cb + 1) * CW], toks[me, cb * TOK:(cb + 1) * TOK, :], (((1,), (1,)), ((), ())), preferred_element_type=F32)
    expert_iota = lax.broadcasted_iota(jnp.int32, (NEXP, TOK), 0)
    chosen = jnp.concatenate([jnp.sum(jnp.where(expert_iota == ids[j:j + 1, :], logits, 0.0), axis=0, keepdims=True) for j in range(TOPK)], axis=0)
    raised = jnp.exp(chosen - jnp.max(chosen, axis=0, keepdims=True))
    route[me, 0:TOPK, :] = (ids[...] * CAP + slots[...]).astype(F32)
    route[me, TOPK:2 * TOPK, :] = raised / jnp.sum(raised, axis=0, keepdims=True)

    pl.semaphore_wait(barrier, DEVS - 1)
    for cb in range(NCB):
        ag_copy(me, cb, 0).start()
        ag_copy(me, (cb + 2) % NCB, 1).start()
        ag_copy(me, cb, 2).start()

    row_i = lax.broadcasted_iota(jnp.int32, (TOK, TOK), 0)
    col_i = lax.broadcasted_iota(jnp.int32, (TOK, TOK), 1)
    causal = row_i >= col_i

    def rope_into(dst, vals):
        for h in range(CW // HEAD):
            part = vals[:, h * HEAD:(h + 1) * HEAD]
            turned = part * cos_t[...] + pltpu.roll(part, HEAD // 2, 1) * sin_t[...]
            dst[:, h * HEAD:(h + 1) * HEAD] = turned.astype(BF16)

    def attn_group(hg, carry):
        g = G_QKV + hg * 3
        slot = ready(g)
        rope_into(qs, dot(xn[...], ring[slot]))
        done(g)

        @pl.when(hg == 0)
        def _():
            for step in range(1, DEVS):
                rt_copy(me, step).start()

        slot = ready(g + 1)
        rope_into(ks, dot(xn[...], ring[slot]))
        done(g + 1)
        slot = ready(g + 2)
        vs[...] = dot(xn[...], ring[slot]).astype(BF16)
        done(g + 2)
        for h in range(CW // HEAD):
            cols = slice(h * HEAD, (h + 1) * HEAD)
            scores = lax.dot_general(qs[:, cols], ks[:, cols], (((1,), (1,)), ((), ())), preferred_element_type=F32) * HEAD ** -0.5
            scores = jnp.where(causal, scores, -jnp.inf)
            expd = jnp.exp(scores - jnp.max(scores, axis=-1, keepdims=True))
            prob = (expd / jnp.sum(expd, axis=-1, keepdims=True)).astype(BF16)
            ctx[:, pl.ds(pl.multiple_of(hg * CW + h * HEAD, HEAD), HEAD)] = dot(prob, vs[:, cols]).astype(BF16)
        return carry

    lax.fori_loop(0, NCB, attn_group, 0)

    def out_block(n, carry):
        g = G_OUT + n
        slot = ready(g)
        cols = aligned(n, CW)
        a_s[:, cols] = (hid[:, cols].astype(F32) + dot(ctx[...], ring[slot])).astype(BF16)
        done(g)
        return carry

    lax.fori_loop(0, N_OUT, out_block, 0)
    a_f = a_s[...].astype(F32)
    inv_rms = lax.rsqrt(jnp.mean(a_f * a_f, axis=-1, keepdims=True) + RMS_EPS)
    for lt in range(DM // LANE):
        cols = slice(lt * LANE, (lt + 1) * LANE)
        xn[:, cols] = (a_s[:, cols].astype(F32) * inv_rms * ffn_norm[lt:lt + 1, :].astype(F32)).astype(BF16)

    def forward(src, cb, links):
        ag_copy(src, cb, 2).wait_recv()
        for link in links:
            ag_copy(src, cb, link).start()

    for cb in range(2):
        forward(src_x, cb, (1, 2))
        forward(src_y, cb + 2, (0, 2))

    def ffn_pair(g, col):
        slot = ready(g)
        z_gate = dot(xn[...], ring[slot])
        done(g)
        slot = ready(g + 1)
        z_up = dot(xn[...], ring[slot])
        done(g + 1)
        hff[:, aligned(col, CW)] = silu_mul(z_gate, z_up)

    def ffn_early(i, carry):
        ffn_pair(G_FFA + 2 * i, i)
        return carry

    lax.fori_loop(0, FF_EARLY, ffn_early, 0)

    def dispatch(src, carry):
        want = lax.broadcasted_iota(jnp.int32, (ROWS, TOK), 0).astype(F32) + (me * ROWS).astype(F32)
        pick = jnp.zeros((ROWS, TOK), F32)
        gate = jnp.zeros((ROWS, TOK), F32)
        for j in range(TOPK):
            hit = route[src, j:j + 1, :] == want
            pick = jnp.where(hit, 1.0, pick)
            gate = jnp.where(hit, route[src, TOPK + j:TOPK + j + 1, :], gate)
        gate_t = jnp.transpose(gate)
        high = gate_t.astype(BF16)
        rest = gate_t - high.astype(F32)
        mid = rest.astype(BF16)
        low = (rest - mid.astype(F32)).astype(BF16)
        gates[src, 0:TOK, :] = high
        gates[src, TOK:2 * TOK, :] = mid
        gates[src, 2 * TOK:3 * TOK, :] = low
        pick = pick.astype(BF16)
        for cb in range(NCB):
            rows = dot(pick, toks[src, cb * TOK:(cb + 1) * TOK, :]).astype(BF16)
            for e in range(LOCAL):
                disp[e, pl.ds(pl.multiple_of(src * CAP, 16), CAP), cb * CW:(cb + 1) * CW] = rows[e * CAP:(e + 1) * CAP, :]
        return carry

    def arrived(src):
        for cb in range(NCB):
            ag_copy(src, cb, 2).wait_recv()

    def dispatch_two(one, two):
        lax.fori_loop(0, 2, lambda i, carry: dispatch(one + i * (two - one), carry), 0)

    for step in range(1, DEVS):
        rt_copy((me + step) % DEVS, step).wait_recv()
    arrived(sib)
    dispatch_two(me, sib)
    for cb in range(2):
        forward(src_x, cb + 2, (2,))
        forward(src_y, cb, (2,))
    dispatch_two(src_x, src_y)
    sib_x, sib_y, sib_d = (c * 2 + 1 - core for c in (chip_x, chip_y, chip_d))
    arrived(sib_x)
    arrived(sib_y)
    dispatch_two(sib_x, sib_y)
    for cb in (0, 2, 1, 3):
        forward(src_d, cb, (2,))
    arrived(sib_d)
    dispatch_two(src_d, sib_d)

    for cb in range(NCB):
        for link in range(3):
            ag_copy(me, cb, link).wait_send()
        for src in (src_x, src_y, src_d):
            ag_copy(src, cb, 2).wait_send()
    for cb in range(2):
        ag_copy(src_x, cb, 1).wait_send()
        ag_copy(src_y, cb + 2, 0).wait_send()
    for step in range(1, DEVS):
        rt_copy(me, step).wait_send()

    def expert_up(i, carry):
        g = G_EGU + 2 * i
        expert, col = i // 2, i % 2
        slot = ready(g)
        slot_up = ready(g + 1)
        for half in range(2):
            cols = slice(half * 256, (half + 1) * 256)
            z_gate = dot(disp[expert], ring[slot, :, cols])
            z_up = dot(disp[expert], ring[slot_up, :, cols])
            hexp[expert, :, pl.ds(pl.multiple_of(col * CW + half * 256, 256), 256)] = silu_mul(z_gate, z_up)
        done(g)
        done(g + 1)
        return carry

    lax.fori_loop(0, 2 * LOCAL, expert_up, 0)

    def fold(b, c):
        s0_copy(b, c).wait_recv()
        pown[b, c] = pown[b, c] + recv0[b, c]

    def fold_others(b):
        s0_copy(b, chip).start()
        for c in (chip_d, chip_x, chip_y):
            fold(b, c)

    def send1_fold_own(b):
        send1(b)
        fold(b, chip)

    def send1(b):
        for which in (1, 0):
            for half in range(2):
                s1_copy(b, half, which).start()

    def fold1(b):
        for half in range(2):
            rows = slice(half * HALF, (half + 1) * HALF)
            for which, dest in ((1, second_chip[half]), (0, chip)):
                s1_copy(b, half, which).wait_recv()
                pown[b, dest, rows, :] = pown[b, dest, rows, :] + recv1[b, half, which]

    def send2(b):
        for half in range(2):
            s2_copy(b, half).start()

    def down_block(b, carry):
        def down_pair(pair, inner):
            g = G_EDN + b * 4 + pair
            slot = ready(g)
            for i in range(2):
                e = pair * 2 + i
                y = dot(hexp[e], ring[slot, i * EFF:(i + 1) * EFF, :]).astype(BF16)
                for s in range(DEVS):
                    toks[s, pl.ds(pl.multiple_of(e * CAP, 16), CAP), :] = y[s * CAP:(s + 1) * CAP, :]
            done(g)

            def at(first, step):
                return pl.when(jnp.logical_and(b >= first, pair == step))

            @at(1, 0)
            def _():
                fold_others(b - 1)

            @at(1, 1)
            def _():
                send1_fold_own(b - 1)

            @at(2, 3)
            def _():
                fold1(b - 2)
            return inner

        lax.fori_loop(0, LOCAL // 2, down_pair, 0)

        def combine(s):
            parts = dot(gates[s], toks[s, 0:ROWS, :])
            return parts[0:TOK] + parts[TOK:2 * TOK] + parts[2 * TOK:3 * TOK]

        @pl.when(b >= 2)
        def _():
            send2(b - 2)
            for c in range(4):
                s0_copy(b - 2, c).wait_send()

        last = None
        for c in (chip_d, chip_x, chip_y, chip):
            psib[b % 2, c] = combine(c * 2 + 1 - core)
            if last is not None:
                s0_copy(b, last).start()
            pown[b, c] = combine(c * 2 + core)
            last = c
        return carry

    lax.fori_loop(0, NCB, down_block, 0)

    def ffn_late(i, carry):
        ffn_pair(G_FFB + 2 * i, FF_EARLY + i)

        for step, act in (
                (0, lambda: fold_others(NCB - 1)), (1, lambda: send1_fold_own(NCB - 1)), (2, lambda: fold1(NCB - 2)),
                (3, lambda: send2(NCB - 2)), (N_LATE - 2, lambda: fold1(NCB - 1)), (N_LATE - 1, lambda: send2(NCB - 1))):
            pl.when(i == step)(act)
        return carry

    lax.fori_loop(0, N_LATE, ffn_late, 0)

    def out_copy(n):
        cols = aligned(n, CW)
        return pltpu.make_async_copy(obuf.at[:, cols], out.at[:, cols], out_sem.at[n])

    def down_out(n, carry):
        cols = aligned(n, CW)
        for kk in range(FF // DM):
            g = G_FDN + n * 4 + kk
            slot = ready(g)
            part = dot(hff[:, kk * DM:(kk + 1) * DM], ring[slot])
            if kk == 0:
                facc[...] = part
            else:
                facc[...] = facc[...] + part

            done(g)
            if kk == 1:
                @pl.when(n > 0)
                def _():
                    out_copy(n - 1).start()
        for half in range(2):
            rows = slice(half * HALF, (half + 1) * HALF)
            s2_copy(n, half).wait_recv()
            moe = pown[n, chip, rows, :] + recv2[n, half]
            obuf[rows, cols] = (a_s[rows, cols].astype(F32) + facc[rows, :] + moe).astype(BF16)
        return carry

    lax.fori_loop(0, NCB, down_out, 0)

    for b in range(NCB):
        for half in range(2):
            s1_copy(b, half, 0).wait_send()
            s1_copy(b, half, 1).wait_send()
            s2_copy(b, half).wait_send()
    for b in (NCB - 2, NCB - 1):
        for c in range(4):
            s0_copy(b, c).wait_send()
    out_copy(NCB - 1).start()
    for n in range(NCB):
        out_copy(n).wait()


def rope_tables():
    half = HEAD // 2
    inv_freq = np.float32(ROPE_BASE) ** (np.float32(-2.0) * np.arange(half, dtype=np.float32) / np.float32(HEAD))
    angles = np.arange(TOK, dtype=np.float32)[:, None] * inv_freq[None, :].astype(np.float32)
    cos_h, sin_h = np.cos(angles).astype(np.float32), np.sin(angles).astype(np.float32)
    return np.concatenate([cos_h, cos_h], axis=1), np.concatenate([-sin_h, sin_h], axis=1)


def solution(mesh):
    row_spec = P(('dp', 'ep'), None, None)
    vec_spec = P(None)
    mat_spec = P(None, None)
    cube_spec = P(None, None, None)
    expert_spec = P('ep', None, None)
    vmem = pl.BlockSpec(memory_space=pltpu.VMEM)
    hbm = pl.BlockSpec(memory_space=pl.ANY)

    def per_device(hidden, expert_ids, slot_ids, attn_norm, w_query, w_key, w_value, w_out, ffn_norm, ffn_gate, ffn_up, ffn_down, moe_norm, w_router, exp_gate, exp_up, exp_down):
        cos_t, sin_t = rope_tables()
        dma = pltpu.SemaphoreType.DMA
        call = pl.pallas_call(
            kernel,
            out_shape=jax.ShapeDtypeStruct((TOK, DM), BF16),
            in_specs=[vmem] * 9 + [hbm] * 10,
            out_specs=hbm,
            scratch_shapes=[
                pltpu.VMEM((NSLOT, DM, CW), BF16),
                pltpu.VMEM((DEVS, NCB * TOK, CW), BF16),
                pltpu.VMEM((LOCAL, DEVS * CAP, DM), BF16),
                pltpu.VMEM((LOCAL, DEVS * CAP, EFF), BF16),
                pltpu.VMEM((NCB, 4, TOK, CW), F32),
                pltpu.VMEM((2, 4, TOK, CW), F32),
                pltpu.VMEM((NCB, 4, TOK, CW), F32),
                pltpu.VMEM((NCB, 2, 2, HALF, CW), F32),
                pltpu.VMEM((NCB, 2, HALF, CW), F32),
                pltpu.VMEM((DEVS, 3 * TOK, ROWS), BF16),
                pltpu.VMEM((DEVS, 2 * TOPK, TOK), F32),
                pltpu.VMEM((TOK, DM), BF16),
                pltpu.VMEM((TOK, DM), BF16),
                pltpu.VMEM((TOK, DM), BF16),
                pltpu.VMEM((TOK, FF), BF16),
                pltpu.VMEM((TOK, CW), F32),
                pltpu.VMEM((TOK, CW), BF16),
                pltpu.VMEM((TOK, CW), BF16),
                pltpu.VMEM((TOK, CW), BF16),
                pltpu.VMEM((TOK, DM), BF16),
                dma((NSLOT,)), dma((3, DEVS, NCB)), dma((DEVS, NCB)), dma((DEVS,)), dma((DEVS,)),
                dma((2, 4)), dma((NCB, 4)), dma((NCB, 2, 2)), dma((NCB, 2, 2)), dma((NCB, 2)), dma((NCB, 2)), dma((NCB,)),
            ],
            compiler_params=pltpu.CompilerParams(collective_id=0, has_side_effects=True, vmem_limit_bytes=67043328),
            cost_estimate=pl.CostEstimate(flops=56_000_000_000, bytes_accessed=240_000_000, transcendentals=0),
        )
        res = call(
            hidden.reshape(TOK, DM), expert_ids.reshape(TOK, TOPK).T, slot_ids.reshape(TOK, TOPK).T,
            attn_norm.reshape(DM // LANE, LANE), ffn_norm.reshape(DM // LANE, LANE), moe_norm.reshape(DM // LANE, LANE), w_router.T, cos_t, sin_t,
            w_query, w_key, w_value, w_out.reshape(DM, DM), ffn_gate, ffn_up, ffn_down, exp_gate, exp_up, exp_down)
        return res.reshape(hidden.shape)

    return jax.shard_map(per_device, mesh=mesh, in_specs=(row_spec, row_spec, row_spec, vec_spec, mat_spec, mat_spec, mat_spec, cube_spec, vec_spec, mat_spec, mat_spec, mat_spec, vec_spec, mat_spec, expert_spec, expert_spec, expert_spec), out_specs=row_spec, check_vma=False)
```

```python
import functools

import jax
import jax.numpy as jnp
import numpy as np
from jax import lax
from jax.experimental import pallas as pl
from jax.experimental.pallas import tpu as pltpu
from jax.sharding import PartitionSpec as P

RMS_EPS = 1e-6
ROPE_BASE = 10000.0
F32 = jnp.float32
BF16 = jnp.bfloat16

DEVS = 8
TOK = 128
HALF = TOK // 2
DM = 2048
HEAD = 128
FF = 8192
LOCAL = 8
FOLD1_AT = ((3, 0), (4, 1), (6, 2), (7, 3))
EFF = 1024
TOPK = 8
LANE = 128
CAP = 48
ROWS = LOCAL * CAP
NEXP = DEVS * LOCAL
CW = 512
NCB = DM // CW
BW = 256
NBW = DM // BW
FF_PAIRS = FF // 2 // CW
NSLOT = 8
FF_EARLY = 1
FF_MID = 0

N_QKV = 12
N_OUT = 4
N_FFA = 2 * (FF_EARLY + FF_MID)
N_EGU = 4 * LOCAL
N_EDN = NBW * (LOCAL // 4)
N_LATE = FF_PAIRS - FF_EARLY - FF_MID
N_FFB = 2 * N_LATE
N_FK = FF // 2 // DM
N_FDN = NCB * N_FK
G_QKV = 0
G_OUT = G_QKV + N_QKV
G_FFA = G_OUT + N_OUT
G_EGU = G_FFA + N_FFA
G_EDN = G_EGU + N_EGU
G_FFB = G_EDN + N_EDN
G_FDN = G_FFB + N_FFB
G_END = G_FDN + N_FDN


def aligned(index, size):
    return pl.ds(pl.multiple_of(index * size, size), size)


def dot(lhs, rhs):
    return jnp.dot(lhs, rhs, preferred_element_type=F32)


def silu_mul(z_gate, z_up):
    return (jax.nn.silu(z_gate) * z_up).astype(BF16)


def kernel(hid, ids, slots, attn_norm, ffn_norm, moe_norm, w_router, cos_t, sin_t,
           w_query, w_key, w_value, w_out, ffn_gate, ffn_up, ffn_down, exp_gate, exp_up, exp_down,
           out,
           ring, toks, disp, hexp, pown, psib, recv0, recv1, recv2, gates, route, ctx, xn, xx, fsend, frecv, a_s, hff, facc, qs, ks, vs, obuf,
           ring_sem, ag_send, ag_recv, rt_send, rt_recv, s0_send, s0_recv, s1_send, s1_recv, s2_send, s2_recv, x_send, x_recv, f_send, f_recv, out_sem):
    me = lax.axis_index("ep")
    chip = me // 2
    core = me % 2
    sib = chip * 2 + 1 - core
    chip_x, chip_y, chip_d = chip + 1 - 2 * (chip % 2), (chip + 2) % 4, 3 - chip
    src_x, src_y, src_d = chip_x * 2 + core, chip_y * 2 + core, chip_d * 2 + core

    def start(g, slot):
        def fetch(src, part=None):
            dst = ring.at[slot] if part is None else ring.at[(slot,) + part]
            pltpu.make_async_copy(src, dst, ring_sem.at[slot]).start()

        def within(lo, hi):
            return pl.when(jnp.logical_and(g >= lo, g < hi))

        @within(G_QKV, G_OUT)
        def _():
            col, kind = g // 3, g % 3
            for which, mat in enumerate((w_query, w_key, w_value)):
                @pl.when(kind == which)
                def _():
                    fetch(mat.at[:, aligned(col, CW)])

        @within(G_OUT, G_FFA)
        def _():
            fetch(w_out.at[:, aligned(g - G_OUT, CW)])

        def ff_pair(local, first):
            col, kind = core * FF_PAIRS + first + local // 2, local % 2

            @pl.when(kind == 0)
            def _():
                fetch(ffn_gate.at[:, aligned(col, CW)])

            @pl.when(kind == 1)
            def _():
                fetch(ffn_up.at[:, aligned(col, CW)])

        @within(G_FFA, G_EGU)
        def _():
            ff_pair(g - G_FFA, 0)

        @within(G_EGU, G_EDN)
        def _():
            local = g - G_EGU
            expert, col, kind = local // 4, (local // 2) % 2, local % 2

            @pl.when(kind == 0)
            def _():
                fetch(exp_gate.at[expert, :, aligned(col, CW)])

            @pl.when(kind == 1)
            def _():
                fetch(exp_up.at[expert, :, aligned(col, CW)])

        @within(G_EDN, G_FFB)
        def _():
            local = g - G_EDN
            col, quad = local // 2, local % 2
            for i in range(4):
                fetch(exp_down.at[quad * 4 + i, :, aligned(col, BW)], (pl.ds(i // 2 * EFF, EFF), pl.ds(i % 2 * BW, BW)))

        @within(G_FFB, G_FDN)
        def _():
            ff_pair(g - G_FFB, FF_EARLY + FF_MID)

        @within(G_FDN, G_END)
        def _():
            local = g - G_FDN
            fetch(ffn_down.at[aligned(core * N_FK + local % N_FK, DM), aligned(local // N_FK, CW)])

    def ready(g):
        slot = g % NSLOT
        pltpu.make_async_copy(w_query.at[:, pl.ds(0, CW)], ring.at[slot], ring_sem.at[slot]).wait()
        return slot

    def done(g):
        start(g + NSLOT, g % NSLOT)

    def send(src, dst, send_sem, recv_sem, peer):
        return pltpu.make_async_remote_copy(src, dst, send_sem, recv_sem, device_id={"ep": peer}, device_id_type=pl.DeviceIdType.MESH)

    def ag_copy(src, cb, link):
        block = toks.at[src, pl.ds(cb * TOK, TOK)]
        return send(block, block, ag_send.at[link, src, cb], ag_recv.at[src, cb], (src_x, src_y, sib)[link])

    def rt_copy(src, step):
        return send(route.at[src], route.at[src], rt_send.at[step], rt_recv.at[src], (me + step) % DEVS)

    first_dev, second_dev = (src_x, src_y), (src_y, src_x)
    slot_of = {"own": (0, 0), "x": (2, 1), "y": (1, 2), "d": (3, 3)}

    def s0_copy(b, half, late):
        part = pl.ds(0 if late else 2, 2)
        return send(psib.at[b % 2, half, part], recv0.at[b, half, part], s0_send.at[b % 2, half, int(late)], s0_recv.at[b, half, int(late)], sib)

    def s1_copy(b, half):
        return send(pown.at[b, half, pl.ds(2, 2)], recv1.at[b, half], s1_send.at[b, half], s1_recv.at[b, half], first_dev[half])

    def s2_copy(b, half):
        return send(pown.at[b, half, 1], recv2.at[b, half], s2_send.at[b, half], s2_recv.at[b, half], second_dev[half])

    for g in range(NSLOT):
        start(jnp.int32(g), g)
    barrier = pltpu.get_barrier_semaphore()
    for step in range(1, DEVS):
        pl.semaphore_signal(barrier, inc=1, device_id={"ep": (me + step) % DEVS}, device_id_type=pl.DeviceIdType.MESH)

    hid_f = hid[...].astype(F32)
    inv_rms = lax.rsqrt(jnp.mean(hid_f * hid_f, axis=-1, keepdims=True) + RMS_EPS)
    for lt in range(DM // LANE):
        cols = slice(lt * LANE, (lt + 1) * LANE)
        cb, within_cb = divmod(lt * LANE, CW)
        part = hid[:, cols].astype(F32) * inv_rms
        toks[me, cb * TOK:(cb + 1) * TOK, within_cb:within_cb + LANE] = (part * moe_norm[lt:lt + 1, :].astype(F32)).astype(BF16)
        xn[:, cols] = (part * attn_norm[lt:lt + 1, :].astype(F32)).astype(BF16)

    pl.semaphore_wait(barrier, DEVS - 1)
    for cb in range(NCB):
        ag_copy(me, cb, 0).start()
        ag_copy(me, (cb + 2) % NCB, 1).start()
        ag_copy(me, cb, 2).start()

    logits = jnp.zeros((NEXP, TOK), F32)
    for cb in range(NCB):
        logits = logits + lax.dot_general(w_router[:, cb * CW:(cb + 1) * CW], toks[me, cb * TOK:(cb + 1) * TOK, :], (((1,), (1,)), ((), ())), preferred_element_type=F32)
    expert_iota = lax.broadcasted_iota(jnp.int32, (NEXP, TOK), 0)
    chosen = jnp.concatenate([jnp.sum(jnp.where(expert_iota == ids[j:j + 1, :], logits, 0.0), axis=0, keepdims=True) for j in range(TOPK)], axis=0)
    raised = jnp.exp(chosen - jnp.max(chosen, axis=0, keepdims=True))
    route[me, 0:TOPK, :] = (ids[...] * CAP + slots[...]).astype(F32)
    route[me, TOPK:2 * TOPK, :] = raised / jnp.sum(raised, axis=0, keepdims=True)

    def forward(src, cb, links):
        ag_copy(src, cb, 2).wait_recv()
        for link in links:
            ag_copy(src, cb, link).start()

    row_i = lax.broadcasted_iota(jnp.int32, (TOK, TOK), 0)
    col_i = lax.broadcasted_iota(jnp.int32, (TOK, TOK), 1)
    causal = row_i >= col_i

    def rope_into(dst, vals):
        for h in range(CW // HEAD):
            part = vals[:, h * HEAD:(h + 1) * HEAD]
            turned = part * cos_t[...] + pltpu.roll(part, HEAD // 2, 1) * sin_t[...]
            dst[:, h * HEAD:(h + 1) * HEAD] = turned.astype(BF16)

    def attn_group(hg, carry):
        g = G_QKV + hg * 3
        slot = ready(g)
        rope_into(qs, dot(xn[...], ring[slot]))
        done(g)

        @pl.when(hg == 0)
        def _():
            for step in range(1, DEVS):
                rt_copy(me, step).start()

        slot = ready(g + 1)
        rope_into(ks, dot(xn[...], ring[slot]))
        done(g + 1)
        slot = ready(g + 2)
        vs[...] = dot(xn[...], ring[slot]).astype(BF16)
        done(g + 2)
        for h in range(CW // HEAD):
            cols = slice(h * HEAD, (h + 1) * HEAD)
            scores = lax.dot_general(qs[:, cols], ks[:, cols], (((1,), (1,)), ((), ())), preferred_element_type=F32) * HEAD ** -0.5
            scores = jnp.where(causal, scores, -jnp.inf)
            expd = jnp.exp(scores - jnp.max(scores, axis=-1, keepdims=True))
            prob = (expd / jnp.sum(expd, axis=-1, keepdims=True)).astype(BF16)
            ctx[:, pl.ds(pl.multiple_of(hg * CW + h * HEAD, HEAD), HEAD)] = dot(prob, vs[:, cols]).astype(BF16)

        @pl.when(hg >= 2)
        def _():
            forward(src_x, hg - 2, (1, 2))
            forward(src_y, hg, (0, 2))
        return carry

    lax.fori_loop(0, NCB, attn_group, 0)

    def out_block(n, carry):
        g = G_OUT + n
        slot = ready(g)
        cols = aligned(n, CW)
        a_s[:, cols] = (hid[:, cols].astype(F32) + dot(ctx[...], ring[slot])).astype(BF16)
        done(g)
        return carry

    lax.fori_loop(0, N_OUT, out_block, 0)
    a_f = a_s[...].astype(F32)
    inv_rms = lax.rsqrt(jnp.mean(a_f * a_f, axis=-1, keepdims=True) + RMS_EPS)
    for lt in range(DM // LANE):
        cols = slice(lt * LANE, (lt + 1) * LANE)
        xx[aligned(core, TOK), cols] = (a_s[:, cols].astype(F32) * inv_rms * ffn_norm[lt:lt + 1, :].astype(F32)).astype(BF16)
    x_block = xx.at[aligned(core, TOK)]
    x_copy = send(x_block, x_block, x_send, x_recv, sib)

    def ffn_pair(g, col):
        slot = ready(g)
        slot_up = ready(g + 1)
        for half in range(2):
            cols = slice(half * 256, (half + 1) * 256)
            z_gate = dot(xx[...], ring[slot, :, cols])
            z_up = dot(xx[...], ring[slot_up, :, cols])
            hff[:, pl.ds(pl.multiple_of(col * CW + half * 256, 256), 256)] = silu_mul(z_gate, z_up)
        done(g)
        done(g + 1)

    def ffn_early(i, carry):
        ffn_pair(G_FFA + 2 * i, i)
        return carry

    def dispatch(src, carry):
        want = lax.broadcasted_iota(jnp.int32, (ROWS, TOK), 0).astype(F32) + (me * ROWS).astype(F32)
        pick = jnp.zeros((ROWS, TOK), F32)
        gate = jnp.zeros((ROWS, TOK), F32)
        for j in range(TOPK):
            hit = route[src, j:j + 1, :] == want
            pick = jnp.where(hit, 1.0, pick)
            gate = jnp.where(hit, route[src, TOPK + j:TOPK + j + 1, :], gate)
        gate_t = jnp.transpose(gate)
        high = gate_t.astype(BF16)
        rest = gate_t - high.astype(F32)
        mid = rest.astype(BF16)
        low = (rest - mid.astype(F32)).astype(BF16)
        gates[src, 0:TOK, :] = high
        gates[src, TOK:2 * TOK, :] = mid
        gates[src, 2 * TOK:3 * TOK, :] = low
        pick = pick.astype(BF16)
        for cb in range(NCB):
            rows = dot(pick, toks[src, cb * TOK:(cb + 1) * TOK, :]).astype(BF16)
            for e in range(LOCAL):
                disp[e, pl.ds(pl.multiple_of(src * CAP, 16), CAP), cb * CW:(cb + 1) * CW] = rows[e * CAP:(e + 1) * CAP, :]
        return carry

    def arrived(src):
        for cb in range(NCB):
            ag_copy(src, cb, 2).wait_recv()

    def dispatch_two(one, two):
        lax.fori_loop(0, 2, lambda i, carry: dispatch(one + i * (two - one), carry), 0)

    for step in range(1, DEVS):
        rt_copy((me + step) % DEVS, step).wait_recv()
    arrived(sib)
    dispatch_two(me, sib)
    x_copy.start()
    for cb in range(2):
        forward(src_x, cb + 2, (2,))
        forward(src_y, cb, (2,))
    dispatch_two(src_x, src_y)
    x_copy.wait()
    lax.fori_loop(0, FF_EARLY, ffn_early, 0)
    sib_x, sib_y, sib_d = (c * 2 + 1 - core for c in (chip_x, chip_y, chip_d))
    arrived(sib_x)
    arrived(sib_y)
    for cb in (0, 2):
        forward(src_d, cb, (2,))
    dispatch_two(sib_x, sib_y)
    for cb in (1, 3):
        forward(src_d, cb, (2,))
    lax.fori_loop(FF_EARLY, FF_EARLY + FF_MID, ffn_early, 0)
    arrived(sib_d)
    dispatch_two(src_d, sib_d)

    for cb in range(NCB):
        for link in range(3):
            ag_copy(me, cb, link).wait_send()
        for src in (src_x, src_y, src_d):
            ag_copy(src, cb, 2).wait_send()
    for cb in range(2):
        ag_copy(src_x, cb, 1).wait_send()
        ag_copy(src_y, cb + 2, 0).wait_send()
    for step in range(1, DEVS):
        rt_copy(me, step).wait_send()

    def expert_up(expert, carry):
        g = G_EGU + 4 * expert
        held = [ready(g + i) for i in range(4)]
        for quarter in range(2):
            z_gate = dot(disp[expert], ring[held[quarter * 2]])
            z_up = dot(disp[expert], ring[held[quarter * 2 + 1]])
            hexp[expert, :, quarter * 512:(quarter + 1) * 512] = silu_mul(z_gate, z_up)
        for i in range(4):
            done(g + i)
        return carry

    lax.fori_loop(0, LOCAL, expert_up, 0)

    def fold0(b, late):
        for half in range(2):
            s0_copy(b, half, late).wait_recv()
            part = slice(0, 2) if late else slice(2, 4)
            pown[b, half, part] = pown[b, half, part] + recv0[b, half, part]

    def start0(b, late):
        for half in range(2):
            s0_copy(b, half, late).start()

    def send1(b):
        for half in range(2):
            s1_copy(b, half).start()

    def fold1(b):
        for half in range(2):
            s1_copy(b, half).wait_recv()
            pown[b, half, 0:2] = pown[b, half, 0:2] + recv1[b, half]

    def send2(b):
        for half in range(2):
            s2_copy(b, half).start()

    def down_block(b, carry):
        def down_quad(quad):
            g = G_EDN + b * 2 + quad
            slot = ready(g)
            for i in range(4):
                e = quad * 4 + i
                y = dot(hexp[e], ring[slot, i // 2 * EFF:(i // 2 + 1) * EFF, i % 2 * BW:(i % 2 + 1) * BW]).astype(BF16)
                for s in range(DEVS):
                    toks[s, e * CAP:(e + 1) * CAP, 0:BW] = y[s * CAP:(s + 1) * CAP, :]
            done(g)

        def combine(dest, side):
            for name, c in (("d", chip_d), ("x", chip_x), ("y", chip_y), ("own", chip)):
                parts = dot(gates[c * 2 + side], toks[c * 2 + side, 0:ROWS, 0:BW])
                moe = parts[0:TOK] + parts[TOK:2 * TOK] + parts[2 * TOK:3 * TOK]
                for half in range(2):
                    dest[half, slot_of[name][half]] = moe[half * HALF:(half + 1) * HALF]

        down_quad(0)

        @pl.when(b >= 1)
        def _():
            fold0(b - 1, False)

        for step, block in FOLD1_AT:
            pl.when(b == step)(functools.partial(fold1, block))

        @pl.when(b >= 2)
        def _():
            for half in range(2):
                s0_copy(b - 2, half, False).wait_send()
                s0_copy(b - 2, half, True).wait_send()

        down_quad(1)

        @pl.when(b >= 1)
        def _():
            send1(b - 1)
            fold0(b - 1, True)

        for step, block in FOLD1_AT:
            pl.when(b == step)(functools.partial(send2, block))

        combine(psib.at[b % 2], 1 - core)
        start0(b, False)
        combine(pown.at[b], core)
        start0(b, True)
        return carry

    lax.fori_loop(0, NBW, down_block, 0)

    def ffn_late(i, carry):
        ffn_pair(G_FFB + 2 * i, FF_EARLY + FF_MID + i)

        for step, act in (
                (0, lambda: fold0(NBW - 1, False)), (1, lambda: send1(NBW - 1)), (1, lambda: fold1(4)),
                (2, lambda: fold0(NBW - 1, True)), (2, lambda: send2(4)), (3, lambda: fold1(5)), (4, lambda: send2(5)), (5, lambda: fold1(6)), (6, lambda: send2(6))):
            pl.when(i == step)(act)
        return carry

    lax.fori_loop(0, N_LATE, ffn_late, 0)

    def out_copy(n):
        cols = aligned(n, CW)
        return pltpu.make_async_copy(obuf.at[:, cols], out.at[:, cols], out_sem.at[n])

    def f_copy(n):
        return send(fsend.at[n], frecv.at[n], f_send.at[n], f_recv.at[n], sib)

    def ffn_out(n, carry):
        for kk in range(N_FK):
            g = G_FDN + n * N_FK + kk
            slot = ready(g)
            part = dot(hff[:, kk * DM:(kk + 1) * DM], ring[slot])
            done(g)
            if kk == 0:
                facc[...] = part
            else:
                facc[...] = facc[...] + part
        fsend[n] = facc[aligned(1 - core, TOK), :]
        for w in range(CW // BW):
            b = n * (CW // BW) + w
            for half in range(2):
                mine = facc[pl.ds(pl.multiple_of(core * TOK + half * HALF, HALF), HALF), w * BW:(w + 1) * BW]
                pown[b, half, 0] = pown[b, half, 0] + mine
        pl.when(n >= 1)(lambda: f_copy(n - 1).start())
        for step, act in ((0, lambda: fold1(7)), (1, lambda: send2(7))):
            pl.when(n == step)(act)
        return carry

    lax.fori_loop(0, NCB, ffn_out, 0)

    def final(n):
        f_copy(n).wait_recv()
        for w in range(CW // BW):
            b = n * (CW // BW) + w
            cols = slice(b * BW, (b + 1) * BW)
            for half in range(2):
                rows = slice(half * HALF, (half + 1) * HALF)
                s2_copy(b, half).wait_recv()
                total = pown[b, half, 0] + recv2[b, half] + frecv[n, rows, w * BW:(w + 1) * BW]
                obuf[rows, cols] = (a_s[rows, cols].astype(F32) + total).astype(BF16)

    final(0)
    f_copy(NCB - 1).start()
    final(1)
    out_copy(0).start()
    final(2)
    out_copy(1).start()
    for b in range(NBW):
        for half in range(2):
            s1_copy(b, half).wait_send()
            if b < NBW - 1:
                s2_copy(b, half).wait_send()
    for b in (NBW - 2, NBW - 1):
        for half in range(2):
            s0_copy(b, half, False).wait_send()
            s0_copy(b, half, True).wait_send()
    for n in range(NCB):
        f_copy(n).wait_send()
    out_copy(2).start()
    final(3)
    for half in range(2):
        s2_copy(NBW - 1, half).wait_send()
    out_copy(3).start()
    for n in range(NCB):
        out_copy(n).wait()


def rope_tables():
    half = HEAD // 2
    inv_freq = np.float32(ROPE_BASE) ** (np.float32(-2.0) * np.arange(half, dtype=np.float32) / np.float32(HEAD))
    angles = np.arange(TOK, dtype=np.float32)[:, None] * inv_freq[None, :].astype(np.float32)
    cos_h, sin_h = np.cos(angles).astype(np.float32), np.sin(angles).astype(np.float32)
    return np.concatenate([cos_h, cos_h], axis=1), np.concatenate([-sin_h, sin_h], axis=1)


def solution(mesh):
    row_spec = P(('dp', 'ep'), None, None)
    vec_spec = P(None)
    mat_spec = P(None, None)
    cube_spec = P(None, None, None)
    expert_spec = P('ep', None, None)
    vmem = pl.BlockSpec(memory_space=pltpu.VMEM)
    hbm = pl.BlockSpec(memory_space=pl.ANY)

    def per_device(hidden, expert_ids, slot_ids, attn_norm, w_query, w_key, w_value, w_out, ffn_norm, ffn_gate, ffn_up, ffn_down, moe_norm, w_router, exp_gate, exp_up, exp_down):
        cos_t, sin_t = rope_tables()
        dma = pltpu.SemaphoreType.DMA
        call = pl.pallas_call(
            kernel,
            out_shape=jax.ShapeDtypeStruct((TOK, DM), BF16),
            in_specs=[vmem] * 9 + [hbm] * 10,
            out_specs=hbm,
            scratch_shapes=[
                pltpu.VMEM((NSLOT, DM, CW), BF16),
                pltpu.VMEM((DEVS, NCB * TOK, CW), BF16),
                pltpu.VMEM((LOCAL, DEVS * CAP, DM), BF16),
                pltpu.VMEM((LOCAL, DEVS * CAP, EFF), BF16),
                pltpu.VMEM((NBW, 2, 4, HALF, BW), F32),
                pltpu.VMEM((2, 2, 4, HALF, BW), F32),
                pltpu.VMEM((NBW, 2, 4, HALF, BW), F32),
                pltpu.VMEM((NBW, 2, 2, HALF, BW), F32),
                pltpu.VMEM((NBW, 2, HALF, BW), F32),
                pltpu.VMEM((DEVS, 3 * TOK, ROWS), BF16),
                pltpu.VMEM((DEVS, 2 * TOPK, TOK), F32),
                pltpu.VMEM((TOK, DM), BF16),
                pltpu.VMEM((TOK, DM), BF16),
                pltpu.VMEM((2 * TOK, DM), BF16),
                pltpu.VMEM((NCB, TOK, CW), F32),
                pltpu.VMEM((NCB, TOK, CW), F32),
                pltpu.VMEM((TOK, DM), BF16),
                pltpu.VMEM((2 * TOK, FF // 2), BF16),
                pltpu.VMEM((2 * TOK, CW), F32),
                pltpu.VMEM((TOK, CW), BF16),
                pltpu.VMEM((TOK, CW), BF16),
                pltpu.VMEM((TOK, CW), BF16),
                pltpu.VMEM((TOK, DM), BF16),
                dma((NSLOT,)), dma((3, DEVS, NCB)), dma((DEVS, NCB)), dma((DEVS,)), dma((DEVS,)),
                dma((2, 2, 2)), dma((NBW, 2, 2)), dma((NBW, 2)), dma((NBW, 2)), dma((NBW, 2)), dma((NBW, 2)),
                dma(()), dma(()), dma((NCB,)), dma((NCB,)), dma((NCB,)),
            ],
            compiler_params=pltpu.CompilerParams(collective_id=0, has_side_effects=True, vmem_limit_bytes=67043328),
            cost_estimate=pl.CostEstimate(flops=56_000_000_000, bytes_accessed=240_000_000, transcendentals=0),
        )
        res = call(
            hidden.reshape(TOK, DM), expert_ids.reshape(TOK, TOPK).T, slot_ids.reshape(TOK, TOPK).T,
            attn_norm.reshape(DM // LANE, LANE), ffn_norm.reshape(DM // LANE, LANE), moe_norm.reshape(DM // LANE, LANE), w_router.T, cos_t, sin_t,
            w_query, w_key, w_value, w_out.reshape(DM, DM), ffn_gate, ffn_up, ffn_down, exp_gate, exp_up, exp_down)
        return res.reshape(hidden.shape)

    return jax.shard_map(per_device, mesh=mesh, in_specs=(row_spec, row_spec, row_spec, vec_spec, mat_spec, mat_spec, mat_spec, cube_spec, vec_spec, mat_spec, mat_spec, mat_spec, vec_spec, mat_spec, expert_spec, expert_spec, expert_spec), out_specs=row_spec, check_vma=False)
```

```python
import functools

import jax
import jax.numpy as jnp
import numpy as np
from jax import lax
from jax.experimental import pallas as pl
from jax.experimental.pallas import tpu as pltpu
from jax.sharding import PartitionSpec as P

RMS_EPS = 1e-6
ROPE_BASE = 10000.0
F32 = jnp.float32
BF16 = jnp.bfloat16

DEVS = 8
TOK = 128
HALF = TOK // 2
DM = 2048
HEAD = 128
FF = 8192
LOCAL = 8
FOLD1_AT = ((3, 0), (4, 1), (6, 2), (7, 3))
EFF = 1024
TOPK = 8
LANE = 128
CAP = 48
ROWS = LOCAL * CAP
NEXP = DEVS * LOCAL
CW = 512
NCB = DM // CW
BW = 256
NBW = DM // BW
FF_PAIRS = FF // 2 // CW
NSLOT = 8
FF_EARLY = 1
FF_MID = 0

N_QKV = 12
N_OUT = 4
N_FFA = 2 * (FF_EARLY + FF_MID)
N_EGU = 4 * LOCAL
N_EDN = NBW * (LOCAL // 4)
N_LATE = FF_PAIRS - FF_EARLY - FF_MID
N_FFB = 2 * N_LATE
N_FK = FF // 2 // DM
N_FDN = NCB * N_FK
G_QKV = 0
G_OUT = G_QKV + N_QKV
G_FFA = G_OUT + N_OUT
G_EGU = G_FFA + N_FFA
G_EDN = G_EGU + N_EGU
G_FFB = G_EDN + N_EDN
G_FDN = G_FFB + N_FFB
G_END = G_FDN + N_FDN


def aligned(index, size):
    return pl.ds(pl.multiple_of(index * size, size), size)


def dot(lhs, rhs):
    return jnp.dot(lhs, rhs, preferred_element_type=F32)


def silu_mul(z_gate, z_up):
    return (jax.nn.silu(z_gate) * z_up).astype(BF16)


def kernel(hid, ids, slots, attn_norm, ffn_norm, moe_norm, w_router, cos_t, sin_t,
           w_query, w_key, w_value, w_out, ffn_gate, ffn_up, ffn_down, exp_gate, exp_up, exp_down,
           out,
           ring, toks, disp, hexp, pown, psib, recv0, recv1, recv2, gates, route, ctx, xx, fsend, frecv, a_s, hff, facc, qs, ks, vs,
           ring_sem, ag_send, ag_recv, rt_send, rt_recv, s0_send, s0_recv, s1_send, s1_recv, s2_send, s2_recv, x_send, x_recv, f_send, f_recv):
    me = lax.axis_index("ep")
    chip = me // 2
    core = me % 2
    sib = chip * 2 + 1 - core
    chip_x, chip_y, chip_d = chip + 1 - 2 * (chip % 2), (chip + 2) % 4, 3 - chip
    mine = aligned(core, TOK)
    src_x, src_y, src_d = chip_x * 2 + core, chip_y * 2 + core, chip_d * 2 + core

    def start(g, slot):
        def fetch(src, part=None):
            dst = ring.at[slot] if part is None else ring.at[(slot,) + part]
            pltpu.make_async_copy(src, dst, ring_sem.at[slot]).start()

        def within(lo, hi):
            return pl.when(jnp.logical_and(g >= lo, g < hi))

        @within(G_QKV, G_OUT)
        def _():
            col, kind = g // 3, g % 3
            for which, mat in enumerate((w_query, w_key, w_value)):
                @pl.when(kind == which)
                def _():
                    fetch(mat.at[:, aligned(col, CW)])

        @within(G_OUT, G_FFA)
        def _():
            fetch(w_out.at[:, aligned(g - G_OUT, CW)])

        def ff_pair(local, first):
            col, kind = core * FF_PAIRS + first + local // 2, local % 2

            @pl.when(kind == 0)
            def _():
                fetch(ffn_gate.at[:, aligned(col, CW)])

            @pl.when(kind == 1)
            def _():
                fetch(ffn_up.at[:, aligned(col, CW)])

        @within(G_FFA, G_EGU)
        def _():
            ff_pair(g - G_FFA, 0)

        @within(G_EGU, G_EDN)
        def _():
            local = g - G_EGU
            expert, col, kind = local // 4, (local // 2) % 2, local % 2

            @pl.when(kind == 0)
            def _():
                fetch(exp_gate.at[expert, :, aligned(col, CW)])

            @pl.when(kind == 1)
            def _():
                fetch(exp_up.at[expert, :, aligned(col, CW)])

        @within(G_EDN, G_FFB)
        def _():
            local = g - G_EDN
            col, quad = local // 2, local % 2
            for i in range(4):
                fetch(exp_down.at[quad * 4 + i, :, aligned(col, BW)], (pl.ds(i // 2 * EFF, EFF), pl.ds(i % 2 * BW, BW)))

        @within(G_FFB, G_FDN)
        def _():
            ff_pair(g - G_FFB, FF_EARLY + FF_MID)

        @within(G_FDN, G_END)
        def _():
            local = g - G_FDN
            fetch(ffn_down.at[aligned(core * N_FK + local % N_FK, DM), aligned(local // N_FK, CW)])

    def ready(g):
        slot = g % NSLOT
        pltpu.make_async_copy(w_query.at[:, pl.ds(0, CW)], ring.at[slot], ring_sem.at[slot]).wait()
        return slot

    def done(g):
        start(g + NSLOT, g % NSLOT)

    def send(src, dst, send_sem, recv_sem, peer):
        return pltpu.make_async_remote_copy(src, dst, send_sem, recv_sem, device_id={"ep": peer}, device_id_type=pl.DeviceIdType.MESH)

    def ag_copy(src, cb, link, sem):
        block = toks.at[src, pl.ds(cb * TOK, TOK)]
        return send(block, block, ag_send.at[0], ag_recv.at[sem], (src_x, src_y, sib)[link])

    def ag_wait(blocks, sem):
        block = toks.at[0, pl.ds(0, blocks * TOK)]
        send(block, block, ag_send.at[0], ag_recv.at[sem], sib).wait_recv()

    def rt_copy(src, step):
        return send(route.at[src], route.at[src], rt_send.at[0], rt_recv.at[0], (me + step) % DEVS)

    first_dev, second_dev = (src_x, src_y), (src_y, src_x)
    slot_of = {"own": (0, 0), "x": (2, 1), "y": (1, 2), "d": (3, 3)}

    def s0_copy(b, half, late):
        part = pl.ds(0 if late else 2, 2)
        return send(psib.at[b % 2, half, part], recv0.at[b % 4, half, part], s0_send.at[b % 2], s0_recv.at[b, int(late)], sib)

    def s1_copy(b, half):
        return send(pown.at[b, half, pl.ds(2, 2)], recv1.at[b, half], s1_send.at[0], s1_recv.at[b], first_dev[half])

    def s2_copy(b, half):
        return send(pown.at[b, half, 1], recv2.at[b, half], s2_send.at[0], s2_recv.at[b], second_dev[half])

    def wait_sent(block, sem):
        send(block, block, sem, s2_recv.at[0], sib).wait_send()

    def wait_got(block, sem):
        send(block, block, s2_send.at[0], sem, sib).wait_recv()

    for g in range(NSLOT):
        start(jnp.int32(g), g)
    barrier = pltpu.get_barrier_semaphore()
    for step in range(1, DEVS):
        pl.semaphore_signal(barrier, inc=1, device_id={"ep": (me + step) % DEVS}, device_id_type=pl.DeviceIdType.MESH)

    hid_f = hid[...].astype(F32)
    inv_rms = lax.rsqrt(jnp.mean(hid_f * hid_f, axis=-1, keepdims=True) + RMS_EPS)
    for lt in range(DM // LANE):
        cols = slice(lt * LANE, (lt + 1) * LANE)
        cb, within_cb = divmod(lt * LANE, CW)
        part = hid[:, cols].astype(F32) * inv_rms
        toks[me, cb * TOK:(cb + 1) * TOK, within_cb:within_cb + LANE] = (part * moe_norm[lt:lt + 1, :].astype(F32)).astype(BF16)
        xx[mine, cols] = (part * attn_norm[lt:lt + 1, :].astype(F32)).astype(BF16)

    pl.semaphore_wait(barrier, DEVS - 1)
    for cb in range(NCB):
        ag_copy(me, cb, 0, min(cb, 2)).start()
        ag_copy(me, (cb + 2) % NCB, 1, 3 + min(cb, 2)).start()
        ag_copy(me, cb, 2, 8).start()

    logits = jnp.zeros((NEXP, TOK), F32)
    for cb in range(NCB):
        logits = logits + lax.dot_general(w_router[:, cb * CW:(cb + 1) * CW], toks[me, cb * TOK:(cb + 1) * TOK, :], (((1,), (1,)), ((), ())), preferred_element_type=F32)
    expert_iota = lax.broadcasted_iota(jnp.int32, (NEXP, TOK), 0)
    chosen = jnp.concatenate([jnp.sum(jnp.where(expert_iota == ids[j:j + 1, :], logits, 0.0), axis=0, keepdims=True) for j in range(TOPK)], axis=0)
    raised = jnp.exp(chosen - jnp.max(chosen, axis=0, keepdims=True))
    route[me, 0:TOPK, :] = (ids[...] * CAP + slots[...]).astype(F32)
    route[me, TOPK:2 * TOPK, :] = raised / jnp.sum(raised, axis=0, keepdims=True)

    def relay(cb, sem_x, sem_y, sem_d):
        for src, block, link, sem, sem_sib in ((src_x, cb, 1, sem_x, 9), (src_y, cb + 2, 0, sem_y, 10)):
            ag_wait(1, sem)
            ag_copy(src, block, link, sem_d).start()
            ag_copy(src, block, 2, sem_sib).start()

    def forward(src, blocks, sem, sem_sib):
        ag_wait(2, sem)
        for cb in blocks:
            ag_copy(src, cb, 2, sem_sib).start()

    row_i = lax.broadcasted_iota(jnp.int32, (TOK, TOK), 0)
    col_i = lax.broadcasted_iota(jnp.int32, (TOK, TOK), 1)
    causal = row_i >= col_i

    def rope_into(dst, vals):
        for h in range(CW // HEAD):
            part = vals[:, h * HEAD:(h + 1) * HEAD]
            turned = part * cos_t[...] + pltpu.roll(part, HEAD // 2, 1) * sin_t[...]
            dst[:, h * HEAD:(h + 1) * HEAD] = turned.astype(BF16)

    def attn_group(hg, carry):
        g = G_QKV + hg * 3
        slot = ready(g)
        rope_into(qs, dot(xx[mine], ring[slot]))
        done(g)

        @pl.when(hg == 0)
        def _():
            for step in range(1, DEVS):
                rt_copy(me, step).start()

        slot = ready(g + 1)
        rope_into(ks, dot(xx[mine], ring[slot]))
        done(g + 1)
        slot = ready(g + 2)
        vs[...] = dot(xx[mine], ring[slot]).astype(BF16)
        done(g + 2)
        for h in range(CW // HEAD):
            cols = slice(h * HEAD, (h + 1) * HEAD)
            scores = lax.dot_general(qs[:, cols], ks[:, cols], (((1,), (1,)), ((), ())), preferred_element_type=F32) * HEAD ** -0.5
            scores = jnp.where(causal, scores, -jnp.inf)
            expd = jnp.exp(scores - jnp.max(scores, axis=-1, keepdims=True))
            prob = (expd / jnp.sum(expd, axis=-1, keepdims=True)).astype(BF16)
            ctx[:, pl.ds(pl.multiple_of(hg * CW + h * HEAD, HEAD), HEAD)] = dot(prob, vs[:, cols]).astype(BF16)

        @pl.when(hg == 2)
        def _():
            relay(0, 0, 3, 6)

        @pl.when(hg == 3)
        def _():
            relay(1, 1, 4, 7)
        return carry

    lax.fori_loop(0, NCB, attn_group, 0)

    def out_block(n, carry):
        g = G_OUT + n
        slot = ready(g)
        cols = aligned(n, CW)
        a_s[:, cols] = (hid[:, cols].astype(F32) + dot(ctx[...], ring[slot])).astype(BF16)
        done(g)
        return carry

    lax.fori_loop(0, N_OUT, out_block, 0)
    a_f = a_s[...].astype(F32)
    inv_rms = lax.rsqrt(jnp.mean(a_f * a_f, axis=-1, keepdims=True) + RMS_EPS)
    for lt in range(DM // LANE):
        cols = slice(lt * LANE, (lt + 1) * LANE)
        xx[aligned(core, TOK), cols] = (a_s[:, cols].astype(F32) * inv_rms * ffn_norm[lt:lt + 1, :].astype(F32)).astype(BF16)
    x_block = xx.at[aligned(core, TOK)]
    x_copy = send(x_block, x_block, x_send, x_recv, sib)

    def ffn_pair(g, col):
        slot = ready(g)
        slot_up = ready(g + 1)
        z_gate = dot(xx[...], ring[slot])
        z_up = dot(xx[...], ring[slot_up])
        hff[:, aligned(col, CW)] = silu_mul(z_gate, z_up)
        done(g)
        done(g + 1)

    def ffn_early(i, carry):
        ffn_pair(G_FFA + 2 * i, i)
        return carry

    def dispatch(src, carry):
        want = lax.broadcasted_iota(jnp.int32, (ROWS, TOK), 0).astype(F32) + (me * ROWS).astype(F32)
        pick = jnp.zeros((ROWS, TOK), F32)
        gate = jnp.zeros((ROWS, TOK), F32)
        for j in range(TOPK):
            hit = route[src, j:j + 1, :] == want
            pick = jnp.where(hit, 1.0, pick)
            gate = jnp.where(hit, route[src, TOPK + j:TOPK + j + 1, :], gate)
        gate_t = jnp.transpose(gate)
        high = gate_t.astype(BF16)
        rest = gate_t - high.astype(F32)
        mid = rest.astype(BF16)
        low = (rest - mid.astype(F32)).astype(BF16)
        gates[src, 0:TOK, :] = high
        gates[src, TOK:2 * TOK, :] = mid
        gates[src, 2 * TOK:3 * TOK, :] = low
        pick = pick.astype(BF16)
        for cb in range(NCB):
            rows = dot(pick, toks[src, cb * TOK:(cb + 1) * TOK, :]).astype(BF16)
            for e in range(LOCAL):
                disp[e, pl.ds(pl.multiple_of(src * CAP, 16), CAP), cb * CW:(cb + 1) * CW] = rows[e * CAP:(e + 1) * CAP, :]
        return carry

    def dispatch_two(one, two):
        lax.fori_loop(0, 2, lambda i, carry: dispatch(one + i * (two - one), carry), 0)

    wait_got(route.at[pl.ds(0, DEVS - 1)], rt_recv.at[0])
    ag_wait(4, 8)
    dispatch_two(me, sib)
    x_copy.start()
    forward(src_x, (2, 3), 2, 9)
    forward(src_y, (0, 1), 5, 10)
    dispatch_two(src_x, src_y)
    x_copy.wait()
    lax.fori_loop(0, FF_EARLY, ffn_early, 0)
    sib_x, sib_y, sib_d = (c * 2 + 1 - core for c in (chip_x, chip_y, chip_d))
    ag_wait(4, 9)
    ag_wait(4, 10)
    forward(src_d, (0, 2), 6, 11)
    dispatch_two(sib_x, sib_y)
    forward(src_d, (1, 3), 7, 11)
    lax.fori_loop(FF_EARLY, FF_EARLY + FF_MID, ffn_early, 0)
    ag_wait(4, 11)
    dispatch_two(src_d, sib_d)

    wait_sent(toks.at[pl.ds(0, 7)], ag_send.at[0])
    wait_sent(route.at[pl.ds(0, DEVS - 1)], rt_send.at[0])

    def expert_up(expert, carry):
        g = G_EGU + 4 * expert
        held = [ready(g + i) for i in range(4)]
        for quarter in range(2):
            z_gate = dot(disp[expert], ring[held[quarter * 2]])
            z_up = dot(disp[expert], ring[held[quarter * 2 + 1]])
            hexp[expert, :, quarter * 512:(quarter + 1) * 512] = silu_mul(z_gate, z_up)
        for i in range(4):
            done(g + i)
        return carry

    lax.fori_loop(0, LOCAL, expert_up, 0)

    def fold0(b, late):
        wait_got(recv0.at[0, 0], s0_recv.at[b, int(late)])
        for half in range(2):
            part = slice(0, 2) if late else slice(2, 4)
            pown[b, half, part] = pown[b, half, part] + recv0[b % 4, half, part]

    def start0(b, late):
        for half in range(2):
            s0_copy(b, half, late).start()

    def send1(b):
        for half in range(2):
            s1_copy(b, half).start()

    def fold1(b):
        wait_got(recv1.at[b], s1_recv.at[b])
        for half in range(2):
            pown[b, half, 0:2] = pown[b, half, 0:2] + recv1[b, half]

    def send2(b):
        for half in range(2):
            s2_copy(b, half).start()

    def down_block(b, carry):
        def down_quad(quad):
            g = G_EDN + b * 2 + quad
            slot = ready(g)
            for i in range(4):
                e = quad * 4 + i
                y = dot(hexp[e], ring[slot, i // 2 * EFF:(i // 2 + 1) * EFF, i % 2 * BW:(i % 2 + 1) * BW]).astype(BF16)
                for s in range(DEVS):
                    toks[s, e * CAP:(e + 1) * CAP, 0:BW] = y[s * CAP:(s + 1) * CAP, :]
            done(g)

        def combine(dest, side):
            for name, c in (("d", chip_d), ("x", chip_x), ("y", chip_y), ("own", chip)):
                parts = dot(gates[c * 2 + side], toks[c * 2 + side, 0:ROWS, 0:BW])
                moe = parts[0:TOK] + parts[TOK:2 * TOK] + parts[2 * TOK:3 * TOK]
                for half in range(2):
                    dest[half, slot_of[name][half]] = moe[half * HALF:(half + 1) * HALF]

        down_quad(0)

        @pl.when(b >= 1)
        def _():
            fold0(b - 1, False)

        for step, block in FOLD1_AT:
            pl.when(b == step)(functools.partial(fold1, block))

        @pl.when(b >= 2)
        def _():
            wait_sent(psib.at[b % 2], s0_send.at[b % 2])

        down_quad(1)

        @pl.when(b >= 1)
        def _():
            send1(b - 1)
            fold0(b - 1, True)

        for step, block in FOLD1_AT:
            pl.when(b == step)(functools.partial(send2, block))

        combine(psib.at[b % 2], 1 - core)
        start0(b, False)
        combine(pown.at[b], core)
        start0(b, True)
        return carry

    lax.fori_loop(0, NBW, down_block, 0)

    def ffn_late(i, carry):
        ffn_pair(G_FFB + 2 * i, FF_EARLY + FF_MID + i)

        for step, act in (
                (0, lambda: fold0(NBW - 1, False)), (1, lambda: send1(NBW - 1)), (1, lambda: fold1(4)),
                (2, lambda: fold0(NBW - 1, True)), (2, lambda: send2(4)), (3, lambda: fold1(5)), (4, lambda: send2(5)), (5, lambda: fold1(6)), (6, lambda: send2(6))):
            pl.when(i == step)(act)
        return carry

    lax.fori_loop(0, N_LATE, ffn_late, 0)

    def f_copy(n):
        return send(fsend.at[n], frecv.at[n], f_send.at[0], f_recv.at[n], sib)

    def ffn_out(n, carry):
        for kk in range(N_FK):
            g = G_FDN + n * N_FK + kk
            slot = ready(g)
            part = dot(hff[:, kk * DM:(kk + 1) * DM], ring[slot])
            done(g)
            if kk == 0:
                facc[...] = part
            else:
                facc[...] = facc[...] + part
        fsend[n] = facc[aligned(1 - core, TOK), :]
        for w in range(CW // BW):
            b = n * (CW // BW) + w
            for half in range(2):
                own = facc[pl.ds(pl.multiple_of(core * TOK + half * HALF, HALF), HALF), w * BW:(w + 1) * BW]
                pown[b, half, 0] = pown[b, half, 0] + own
        pl.when(n >= 1)(lambda: f_copy(n - 1).start())
        for step, act in ((0, lambda: fold1(7)), (1, lambda: send2(7))):
            pl.when(n == step)(act)
        return carry

    lax.fori_loop(0, NCB, ffn_out, 0)

    def final(n):
        f_copy(n).wait_recv()
        for w in range(CW // BW):
            b = n * (CW // BW) + w
            cols = slice(b * BW, (b + 1) * BW)
            wait_got(recv2.at[b], s2_recv.at[b])
            for half in range(2):
                rows = slice(half * HALF, (half + 1) * HALF)
                total = pown[b, half, 0] + recv2[b, half] + frecv[n, rows, w * BW:(w + 1) * BW]
                out[rows, cols] = (a_s[rows, cols].astype(F32) + total).astype(BF16)

    final(0)
    f_copy(NCB - 1).start()
    final(1)
    final(2)
    wait_sent(pown.at[pl.ds(0, 4)], s1_send.at[0])
    for parity in range(2):
        wait_sent(psib.at[parity], s0_send.at[parity])
    wait_sent(fsend, f_send.at[0])
    final(3)
    wait_sent(pown.at[pl.ds(0, 2)], s2_send.at[0])


def rope_tables():
    half = HEAD // 2
    inv_freq = np.float32(ROPE_BASE) ** (np.float32(-2.0) * np.arange(half, dtype=np.float32) / np.float32(HEAD))
    angles = np.arange(TOK, dtype=np.float32)[:, None] * inv_freq[None, :].astype(np.float32)
    cos_h, sin_h = np.cos(angles).astype(np.float32), np.sin(angles).astype(np.float32)
    return np.concatenate([cos_h, cos_h], axis=1), np.concatenate([-sin_h, sin_h], axis=1)


def solution(mesh):
    row_spec = P(('dp', 'ep'), None, None)
    vec_spec = P(None)
    mat_spec = P(None, None)
    cube_spec = P(None, None, None)
    expert_spec = P('ep', None, None)
    vmem = pl.BlockSpec(memory_space=pltpu.VMEM)
    hbm = pl.BlockSpec(memory_space=pl.ANY)

    def per_device(hidden, expert_ids, slot_ids, attn_norm, w_query, w_key, w_value, w_out, ffn_norm, ffn_gate, ffn_up, ffn_down, moe_norm, w_router, exp_gate, exp_up, exp_down):
        cos_t, sin_t = rope_tables()
        dma = pltpu.SemaphoreType.DMA
        call = pl.pallas_call(
            kernel,
            out_shape=pltpu.VMEM((TOK, DM), BF16),
            in_specs=[vmem] * 9 + [hbm] * 10,
            out_specs=vmem,
            scratch_shapes=[
                pltpu.VMEM((NSLOT, DM, CW), BF16),
                pltpu.VMEM((DEVS, NCB * TOK, CW), BF16),
                pltpu.VMEM((LOCAL, DEVS * CAP, DM), BF16),
                pltpu.VMEM((LOCAL, DEVS * CAP, EFF), BF16),
                pltpu.VMEM((NBW, 2, 4, HALF, BW), F32),
                pltpu.VMEM((2, 2, 4, HALF, BW), F32),
                pltpu.VMEM((4, 2, 4, HALF, BW), F32),
                pltpu.VMEM((NBW, 2, 2, HALF, BW), F32),
                pltpu.VMEM((NBW, 2, HALF, BW), F32),
                pltpu.VMEM((DEVS, 3 * TOK, ROWS), BF16),
                pltpu.VMEM((DEVS, 2 * TOPK, TOK), F32),
                pltpu.VMEM((TOK, DM), BF16),
                pltpu.VMEM((2 * TOK, DM), BF16),
                pltpu.VMEM((NCB, TOK, CW), F32),
                pltpu.VMEM((NCB, TOK, CW), F32),
                pltpu.VMEM((TOK, DM), BF16),
                pltpu.VMEM((2 * TOK, FF // 2), BF16),
                pltpu.VMEM((2 * TOK, CW), F32),
                pltpu.VMEM((TOK, CW), BF16),
                pltpu.VMEM((TOK, CW), BF16),
                pltpu.VMEM((TOK, CW), BF16),
                dma((NSLOT,)), dma((1,)), dma((12,)), dma((1,)), dma((1,)),
                dma((2,)), dma((NBW, 2)), dma((1,)), dma((NBW,)), dma((1,)), dma((NBW,)),
                dma(()), dma(()), dma((1,)), dma((NCB,)),
            ],
            compiler_params=pltpu.CompilerParams(collective_id=0, has_side_effects=True, vmem_limit_bytes=66000000),
            cost_estimate=pl.CostEstimate(flops=56_000_000_000, bytes_accessed=240_000_000, transcendentals=0),
        )
        res = call(
            hidden.reshape(TOK, DM), expert_ids.reshape(TOK, TOPK).T, slot_ids.reshape(TOK, TOPK).T,
            attn_norm.reshape(DM // LANE, LANE), ffn_norm.reshape(DM // LANE, LANE), moe_norm.reshape(DM // LANE, LANE), w_router.T, cos_t, sin_t,
            w_query, w_key, w_value, w_out.reshape(DM, DM), ffn_gate, ffn_up, ffn_down, exp_gate, exp_up, exp_down)
        return res.reshape(hidden.shape)

    return jax.shard_map(per_device, mesh=mesh, in_specs=(row_spec, row_spec, row_spec, vec_spec, mat_spec, mat_spec, mat_spec, cube_spec, vec_spec, mat_spec, mat_spec, mat_spec, vec_spec, mat_spec, expert_spec, expert_spec, expert_spec), out_specs=row_spec, check_vma=False)
```

```python
import functools

import jax
import jax.numpy as jnp
import numpy as np
from jax import lax
from jax.experimental import pallas as pl
from jax.experimental.pallas import tpu as pltpu
from jax.sharding import PartitionSpec as P

RMS_EPS = 1e-6
ROPE_BASE = 10000.0
F32 = jnp.float32
BF16 = jnp.bfloat16

DEVS = 8
TOK = 128
HALF = TOK // 2
DM = 2048
HEAD = 128
FF = 8192
LOCAL = 8
FOLD1_MID = ((5, 2),)
FOLD1_END = ((2, 0), (3, 1), (6, 3), (7, 4))
SEND2_START = ((3, 0), (4, 1), (7, 3))
EFF = 1024
TOPK = 8
LANE = 128
CAP = 48
ROWS = LOCAL * CAP
NEXP = DEVS * LOCAL
CW = 512
NCB = DM // CW
BW = 256
NBW = DM // BW
FF_PAIRS = FF // 2 // CW
NSLOT = 8
FF_EARLY = 1
FF_MID = 0

N_QKV = 12
N_OUT = 4
N_FFA = 2 * (FF_EARLY + FF_MID)
N_EGU = 4 * LOCAL
N_EDN = NBW * (LOCAL // 4)
N_LATE = FF_PAIRS - FF_EARLY - FF_MID
N_FFB = 2 * N_LATE
N_FK = FF // 2 // DM
N_FDN = NCB * N_FK
G_QKV = 0
G_OUT = G_QKV + N_QKV
G_FFA = G_OUT + N_OUT
G_EGU = G_FFA + N_FFA
G_EDN = G_EGU + N_EGU
G_FFB = G_EDN + N_EDN
G_FDN = G_FFB + N_FFB
G_END = G_FDN + N_FDN


def aligned(index, size):
    return pl.ds(pl.multiple_of(index * size, size), size)


def dot(lhs, rhs):
    return jnp.dot(lhs, rhs, preferred_element_type=F32)


def silu_mul(z_gate, z_up):
    return (jax.nn.silu(z_gate) * z_up).astype(BF16)


def kernel(hid_h, ids_h, slots_h, attn_norm_h, ffn_norm_h, moe_norm_h, w_router_h, cos_h, sin_h,
           w_query, w_key, w_value, w_out, ffn_gate, ffn_up, ffn_down, exp_gate, exp_up, exp_down,
           out,
           ring, toks, disp, hexp, pown, psib, recv0, recv1, recv2, gates, picks, route, ctx, xx, fsend, frecv, a_s, hff, facc, qs, ks, vs,
           ring_sem, ag_send, ag_recv, rt_send, rt_recv, s0_send, s0_recv, s1_send, s1_recv, s2_send, s2_recv, x_send, x_recv, f_send, f_recv, in_sem,
           hid, ids, slots, attn_norm, ffn_norm, moe_norm, w_router, cos_t, sin_t):
    me = lax.axis_index("ep")
    chip = me // 2
    core = me % 2
    sib = chip * 2 + 1 - core
    chip_x, chip_y, chip_d = chip + 1 - 2 * (chip % 2), (chip + 2) % 4, 3 - chip
    mine = aligned(core, TOK)
    src_x, src_y, src_d = chip_x * 2 + core, chip_y * 2 + core, chip_d * 2 + core

    def fetch(slot, src, part=None):
        dst = ring.at[slot] if part is None else ring.at[(slot,) + part]
        pltpu.make_async_copy(src, dst, ring_sem.at[slot]).start()

    def fetch_ffn(slot, pair, mat):
        fetch(slot, mat.at[:, aligned(core * FF_PAIRS + pair, CW)])

    def fetch_expert(slot, expert, col, mat):
        fetch(slot, mat.at[expert, :, aligned(col, CW)])

    def fetch_down(slot, col, quad):
        for i in range(4):
            fetch(slot, exp_down.at[quad * 4 + i, :, aligned(col, BW)], (pl.ds(i // 2 * EFF, EFF), pl.ds(i % 2 * BW, BW)))

    def fetch_ffn_down(slot, n, kk):
        fetch(slot, ffn_down.at[aligned(core * N_FK + kk, DM), aligned(n, CW)])

    def start(g, slot):
        def within(lo, hi):
            return pl.when(jnp.logical_and(g >= lo, g < hi))

        @within(G_QKV, G_OUT)
        def _():
            for which, mat in enumerate((w_query, w_key, w_value)):
                pl.when(g % 3 == which)(lambda mat=mat: fetch(slot, mat.at[:, aligned(g // 3, CW)]))

        @within(G_OUT, G_FFA)
        def _():
            fetch(slot, w_out.at[:, aligned(g - G_OUT, CW)])

        @within(G_FFA, G_EGU)
        def _():
            local = g - G_FFA
            for which, mat in enumerate((ffn_gate, ffn_up)):
                pl.when(local % 2 == which)(lambda mat=mat: fetch_ffn(slot, local // 2, mat))

        @within(G_EGU, G_EDN)
        def _():
            local = g - G_EGU
            for which, mat in enumerate((exp_gate, exp_up)):
                pl.when(local % 2 == which)(lambda mat=mat: fetch_expert(slot, local // 4, local // 2 % 2, mat))

    def ready(g):
        slot = g % NSLOT
        pltpu.make_async_copy(w_query.at[:, pl.ds(0, CW)], ring.at[slot], ring_sem.at[slot]).wait()
        return slot

    def done(g):
        start(g + NSLOT, g % NSLOT)

    def send(src, dst, send_sem, recv_sem, peer):
        return pltpu.make_async_remote_copy(src, dst, send_sem, recv_sem, device_id={"ep": peer}, device_id_type=pl.DeviceIdType.MESH)

    def ag_copy(src, cb, link, sem):
        block = toks.at[src, pl.ds(cb * TOK, TOK)]
        return send(block, block, ag_send.at[0], ag_recv.at[sem], (src_x, src_y, sib)[link])

    def ag_wait(blocks, sem):
        block = toks.at[0, pl.ds(0, blocks * TOK)]
        send(block, block, ag_send.at[0], ag_recv.at[sem], sib).wait_recv()

    def rt_copy(src, step):
        return send(route.at[src], route.at[src], rt_send.at[0], rt_recv.at[0], (me + step) % DEVS)

    first_dev, second_dev = (src_x, src_y), (src_y, src_x)
    slot_of = {"own": (0, 0), "x": (2, 1), "y": (1, 2), "d": (3, 3)}

    def s0_copy(b, half, late):
        part = pl.ds(0 if late else 2, 2)
        return send(psib.at[b % 2, half, part], recv0.at[b % 4, half, part], s0_send.at[b % 2], s0_recv.at[b, int(late)], sib)

    def s1_copy(b, half):
        return send(pown.at[b, half, pl.ds(2, 2)], recv1.at[b, half], s1_send.at[0], s1_recv.at[b], first_dev[half])

    def s2_copy(b, half):
        return send(pown.at[b, half, 1], recv2.at[b, half], s2_send.at[0], s2_recv.at[b], second_dev[half])

    def wait_sent(block, sem):
        send(block, block, sem, s2_recv.at[0], sib).wait_send()

    def wait_got(block, sem):
        send(block, block, s2_send.at[0], sem, sib).wait_recv()

    loads = {name: pltpu.make_async_copy(src, dst, in_sem.at[i]) for i, (name, src, dst) in enumerate((
        ("hid", hid_h, hid), ("moe_norm", moe_norm_h, moe_norm), ("attn_norm", attn_norm_h, attn_norm),
        ("w_router", w_router_h, w_router), ("ids", ids_h, ids), ("slots", slots_h, slots),
        ("cos", cos_h, cos_t), ("sin", sin_h, sin_t), ("ffn_norm", ffn_norm_h, ffn_norm)))}

    def loaded(*names):
        for name in names:
            loads[name].wait()

    barrier = pltpu.get_barrier_semaphore()
    for step in range(1, DEVS):
        pl.semaphore_signal(barrier, inc=1, device_id={"ep": (me + step) % DEVS}, device_id_type=pl.DeviceIdType.MESH)
    for load in loads.values():
        load.start()
    loaded("hid", "moe_norm", "attn_norm", "w_router", "ids", "slots", "cos", "sin", "ffn_norm")
    for g in range(NSLOT):
        start(jnp.int32(g), g)

    hid_f = hid[...].astype(F32)
    inv_rms = lax.rsqrt(jnp.mean(hid_f * hid_f, axis=-1, keepdims=True) + RMS_EPS)
    for lt in range(DM // LANE):
        cols = slice(lt * LANE, (lt + 1) * LANE)
        cb, within_cb = divmod(lt * LANE, CW)
        part = hid[:, cols].astype(F32) * inv_rms
        toks[me, cb * TOK:(cb + 1) * TOK, within_cb:within_cb + LANE] = (part * moe_norm[lt:lt + 1, :].astype(F32)).astype(BF16)
        xx[mine, cols] = (part * attn_norm[lt:lt + 1, :].astype(F32)).astype(BF16)

    pl.semaphore_wait(barrier, DEVS - 1)
    for cb in range(NCB):
        ag_copy(me, cb, 0, min(cb, 2)).start()
        ag_copy(me, (cb + 2) % NCB, 1, 3 + min(cb, 2)).start()
        ag_copy(me, cb, 2, 8).start()

    logits = jnp.zeros((NEXP, TOK), F32)
    for cb in range(NCB):
        logits = logits + lax.dot_general(w_router[:, cb * CW:(cb + 1) * CW], toks[me, cb * TOK:(cb + 1) * TOK, :], (((1,), (1,)), ((), ())), preferred_element_type=F32)
    expert_iota = lax.broadcasted_iota(jnp.int32, (NEXP, TOK), 0)
    chosen = jnp.concatenate([jnp.sum(jnp.where(expert_iota == ids[j:j + 1, :], logits, 0.0), axis=0, keepdims=True) for j in range(TOPK)], axis=0)
    raised = jnp.exp(chosen - jnp.max(chosen, axis=0, keepdims=True))
    route[me, 0:TOPK, :] = (ids[...] * CAP + slots[...]).astype(F32)
    route[me, TOPK:2 * TOPK, :] = raised / jnp.sum(raised, axis=0, keepdims=True)

    def relay(cb, sem_x, sem_y, sem_d):
        for src, block, link, sem, sem_sib in ((src_x, cb, 1, sem_x, 9), (src_y, cb + 2, 0, sem_y, 10)):
            ag_wait(1, sem)
            ag_copy(src, block, link, sem_d).start()
            ag_copy(src, block, 2, sem_sib).start()

    def forward(src, blocks, sem, sem_sib):
        ag_wait(2, sem)
        for cb in blocks:
            ag_copy(src, cb, 2, sem_sib).start()

    row_i = lax.broadcasted_iota(jnp.int32, (TOK, TOK), 0)
    col_i = lax.broadcasted_iota(jnp.int32, (TOK, TOK), 1)
    causal = row_i >= col_i

    def rope_into(dst, vals):
        for h in range(CW // HEAD):
            part = vals[:, h * HEAD:(h + 1) * HEAD]
            turned = part * cos_t[...] + pltpu.roll(part, HEAD // 2, 1) * sin_t[...]
            dst[:, h * HEAD:(h + 1) * HEAD] = turned.astype(BF16)

    def attn_group(hg, carry):
        g = G_QKV + hg * 3
        slot = ready(g)
        rope_into(qs, dot(xx[mine], ring[slot]))
        done(g)

        @pl.when(hg == 0)
        def _():
            for step in range(1, DEVS):
                rt_copy(me, step).start()

        slot = ready(g + 1)
        rope_into(ks, dot(xx[mine], ring[slot]))
        done(g + 1)
        slot = ready(g + 2)
        vs[...] = dot(xx[mine], ring[slot]).astype(BF16)
        done(g + 2)
        for h in range(CW // HEAD):
            cols = slice(h * HEAD, (h + 1) * HEAD)
            scores = lax.dot_general(qs[:, cols], ks[:, cols], (((1,), (1,)), ((), ())), preferred_element_type=F32) * HEAD ** -0.5
            scores = jnp.where(causal, scores, -jnp.inf)
            expd = jnp.exp(scores - jnp.max(scores, axis=-1, keepdims=True))
            prob = (expd / jnp.sum(expd, axis=-1, keepdims=True)).astype(BF16)
            ctx[:, pl.ds(pl.multiple_of(hg * CW + h * HEAD, HEAD), HEAD)] = dot(prob, vs[:, cols]).astype(BF16)

        @pl.when(hg == 2)
        def _():
            relay(0, 0, 3, 6)

        @pl.when(hg == 3)
        def _():
            relay(1, 1, 4, 7)
        return carry

    lax.fori_loop(0, NCB, attn_group, 0)

    def out_block(n, carry):
        g = G_OUT + n
        slot = ready(g)
        cols = aligned(n, CW)
        a_s[:, cols] = (hid[:, cols].astype(F32) + dot(ctx[...], ring[slot])).astype(BF16)
        done(g)
        return carry

    lax.fori_loop(0, N_OUT, out_block, 0)
    a_f = a_s[...].astype(F32)
    inv_rms = lax.rsqrt(jnp.mean(a_f * a_f, axis=-1, keepdims=True) + RMS_EPS)
    for lt in range(DM // LANE):
        cols = slice(lt * LANE, (lt + 1) * LANE)
        xx[aligned(core, TOK), cols] = (a_s[:, cols].astype(F32) * inv_rms * ffn_norm[lt:lt + 1, :].astype(F32)).astype(BF16)
    x_block = xx.at[aligned(core, TOK)]
    x_copy = send(x_block, x_block, x_send, x_recv, sib)

    def ffn_pair(g, col, refill, between=None):
        slot = ready(g)
        slot_up = ready(g + 1)
        if between is not None:
            between()
        z_gate = dot(xx[...], ring[slot])
        z_up = dot(xx[...], ring[slot_up])
        hff[:, aligned(col, CW)] = silu_mul(z_gate, z_up)
        refill(slot, slot_up)

    def ffn_early(i, carry):
        g = G_FFA + 2 * i

        def refill(slot, slot_up):
            done(g)
            done(g + 1)

        ffn_pair(g, i, refill)
        return carry

    def choose(src):
        want = lax.broadcasted_iota(jnp.int32, (ROWS, TOK), 0).astype(F32) + (me * ROWS).astype(F32)
        pick = jnp.zeros((ROWS, TOK), F32)
        gate = jnp.zeros((ROWS, TOK), F32)
        for j in range(TOPK):
            hit = route[src, j:j + 1, :] == want
            pick = jnp.where(hit, 1.0, pick)
            gate = jnp.where(hit, route[src, TOPK + j:TOPK + j + 1, :], gate)
        gate_t = jnp.transpose(gate)
        high = gate_t.astype(BF16)
        rest = gate_t - high.astype(F32)
        mid = rest.astype(BF16)
        low = (rest - mid.astype(F32)).astype(BF16)
        gates[src, 0:TOK, :] = high
        gates[src, TOK:2 * TOK, :] = mid
        gates[src, 2 * TOK:3 * TOK, :] = low
        picks[...] = pick.astype(BF16)

    def place(src):
        for cb in range(NCB):
            rows = dot(picks[...], toks[src, cb * TOK:(cb + 1) * TOK, :]).astype(BF16)
            for e in range(LOCAL):
                disp[e, pl.ds(pl.multiple_of(src * CAP, 16), CAP), cb * CW:(cb + 1) * CW] = rows[e * CAP:(e + 1) * CAP, :]

    def dispatch(src, carry):
        choose(src)
        place(src)
        return carry

    def dispatch_two(one, two):
        lax.fori_loop(0, 2, lambda i, carry: dispatch(one + i * (two - one), carry), 0)

    wait_got(route.at[pl.ds(0, DEVS - 1)], rt_recv.at[0])
    ag_wait(4, 8)
    x_copy.start()
    dispatch_two(me, sib)
    forward(src_x, (2, 3), 2, 9)
    forward(src_y, (0, 1), 5, 10)
    dispatch_two(src_x, src_y)
    x_copy.wait()
    lax.fori_loop(0, FF_EARLY, ffn_early, 0)
    sib_x, sib_y, sib_d = (c * 2 + 1 - core for c in (chip_x, chip_y, chip_d))
    ag_wait(4, 9)
    ag_wait(4, 10)
    forward(src_d, (0, 2), 6, 11)
    dispatch(sib_x, 0)
    forward(src_d, (1, 3), 7, 11)
    dispatch(sib_y, 0)
    lax.fori_loop(FF_EARLY, FF_EARLY + FF_MID, ffn_early, 0)
    dispatch(src_d, 0)
    choose(sib_d)
    ag_wait(4, 11)
    place(sib_d)

    wait_sent(toks.at[pl.ds(0, 7)], ag_send.at[0])
    wait_sent(route.at[pl.ds(0, DEVS - 1)], rt_send.at[0])

    def expert_up(expert, carry):
        g = G_EGU + 4 * expert
        held = [ready(g + i) for i in range(4)]
        for quarter in range(2):
            z_gate = dot(disp[expert], ring[held[quarter * 2]])
            z_up = dot(disp[expert], ring[held[quarter * 2 + 1]])
            hexp[expert, :, quarter * 512:(quarter + 1) * 512] = silu_mul(z_gate, z_up)

        @pl.when(expert < LOCAL - 2)
        def _():
            for i in range(4):
                fetch_expert(held[i], expert + 2, i // 2, (exp_gate, exp_up)[i % 2])

        @pl.when(expert >= LOCAL - 2)
        def _():
            for i in range(4):
                fetch_down(held[i], (expert - (LOCAL - 2)) * 2 + i // 2, i % 2)
        return carry

    lax.fori_loop(0, LOCAL, expert_up, 0)

    def fold0(b, late):
        wait_got(recv0.at[0, 0], s0_recv.at[b, int(late)])
        for half in range(2):
            part = slice(0, 2) if late else slice(2, 4)
            pown[b, half, part] = pown[b, half, part] + recv0[b % 4, half, part]

    def start0(b, late):
        for half in range(2):
            s0_copy(b, half, late).start()

    def send1(b):
        for half in range(2):
            s1_copy(b, half).start()

    def fold1(b):
        wait_got(recv1.at[b], s1_recv.at[b])
        for half in range(2):
            pown[b, half, 0:2] = pown[b, half, 0:2] + recv1[b, half]

    def send2(b):
        for half in range(2):
            s2_copy(b, half).start()

    def down_block(b, carry):
        def down_quad(quad, slot):
            for i in range(4):
                e = quad * 4 + i
                y = dot(hexp[e], ring[slot, i // 2 * EFF:(i // 2 + 1) * EFF, i % 2 * BW:(i % 2 + 1) * BW]).astype(BF16)
                for s in range(DEVS):
                    toks[s, e * CAP:(e + 1) * CAP, 0:BW] = y[s * CAP:(s + 1) * CAP, :]
            pl.when(b < NBW - 4)(lambda: fetch_down(slot, b + 4, quad))
            pl.when(b >= NBW - 4)(lambda: fetch_ffn(slot, FF_EARLY + FF_MID + b - (NBW - 4), (ffn_gate, ffn_up)[quad]))

        def at(table, act):
            for step, block in table:
                pl.when(b == step)(functools.partial(act, block))

        def combine(dest, side):
            for name, c in (("d", chip_d), ("x", chip_x), ("y", chip_y), ("own", chip)):
                parts = dot(gates[c * 2 + side], toks[c * 2 + side, 0:ROWS, 0:BW])
                moe = parts[0:TOK] + parts[TOK:2 * TOK] + parts[2 * TOK:3 * TOK]
                for half in range(2):
                    dest[half, slot_of[name][half]] = moe[half * HALF:(half + 1) * HALF]

        g = G_EDN + b * 2
        slot = ready(g)
        at(SEND2_START, send2)
        down_quad(0, slot)

        @pl.when(b >= 1)
        def _():
            fold0(b - 1, False)

        at(FOLD1_MID, fold1)

        @pl.when(b >= 2)
        def _():
            wait_sent(psib.at[b % 2], s0_send.at[b % 2])

        slot = ready(g + 1)
        pl.when(b >= 1)(lambda: send1(b - 1))
        at(FOLD1_MID, send2)
        down_quad(1, slot)
        pl.when(b >= 1)(lambda: fold0(b - 1, True))
        combine(psib.at[b % 2], 1 - core)
        start0(b, False)
        combine(pown.at[b], core)
        start0(b, True)
        at(FOLD1_END, fold1)
        return carry

    lax.fori_loop(0, NBW, down_block, 0)

    def ffn_late(i, carry):
        g = G_FFB + 2 * i

        def refill(slot, slot_up):
            pair = i + 4

            @pl.when(pair < N_LATE)
            def _():
                fetch_ffn(slot, FF_EARLY + FF_MID + pair, ffn_gate)
                fetch_ffn(slot_up, FF_EARLY + FF_MID + pair, ffn_up)

            @pl.when(pair >= N_LATE)
            def _():
                fetch_ffn_down(slot, pair - N_LATE, 0)
                fetch_ffn_down(slot_up, pair - N_LATE, 1)

        def before():
            for step, act in ((0, lambda: send2(4)), (1, lambda: send1(NBW - 1)), (2, lambda: send2(5)), (5, lambda: send2(6))):
                pl.when(i == step)(act)

        ffn_pair(g, FF_EARLY + FF_MID + i, refill, before)
        for step, act in ((0, lambda: fold0(NBW - 1, False)), (1, lambda: fold0(NBW - 1, True)), (1, lambda: fold1(5)), (4, lambda: fold1(6))):
            pl.when(i == step)(act)
        return carry

    lax.fori_loop(0, N_LATE, ffn_late, 0)

    def f_copy(n):
        return send(fsend.at[n], frecv.at[n], f_send.at[0], f_recv.at[n], sib)

    def ffn_out(n, carry):
        g = G_FDN + n * N_FK
        held = [ready(g + kk) for kk in range(N_FK)]
        pl.when(n == 1)(lambda: send2(NBW - 1))
        facc[...] = sum(dot(hff[:, kk * DM:(kk + 1) * DM], ring[held[kk]]) for kk in range(N_FK))
        fsend[n] = facc[aligned(1 - core, TOK), :]
        for w in range(CW // BW):
            b = n * (CW // BW) + w
            for half in range(2):
                own = facc[pl.ds(pl.multiple_of(core * TOK + half * HALF, HALF), HALF), w * BW:(w + 1) * BW]
                pown[b, half, 0] = pown[b, half, 0] + own
        pl.when(n >= 1)(lambda: f_copy(n - 1).start())
        pl.when(n == 0)(lambda: fold1(NBW - 1))
        return carry

    lax.fori_loop(0, NCB, ffn_out, 0)

    def final(n):
        f_copy(n).wait_recv()
        for w in range(CW // BW):
            b = n * (CW // BW) + w
            cols = slice(b * BW, (b + 1) * BW)
            wait_got(recv2.at[b], s2_recv.at[b])
            for half in range(2):
                rows = slice(half * HALF, (half + 1) * HALF)
                total = pown[b, half, 0] + recv2[b, half] + frecv[n, rows, w * BW:(w + 1) * BW]
                out[rows, cols] = (a_s[rows, cols].astype(F32) + total).astype(BF16)

    final(0)
    f_copy(NCB - 1).start()
    final(1)
    final(2)
    wait_sent(pown.at[pl.ds(0, 4)], s1_send.at[0])
    for parity in range(2):
        wait_sent(psib.at[parity], s0_send.at[parity])
    wait_sent(fsend, f_send.at[0])
    final(3)
    wait_sent(pown.at[pl.ds(0, 2)], s2_send.at[0])


def rope_tables():
    half = HEAD // 2
    inv_freq = np.float32(ROPE_BASE) ** (np.float32(-2.0) * np.arange(half, dtype=np.float32) / np.float32(HEAD))
    angles = np.arange(TOK, dtype=np.float32)[:, None] * inv_freq[None, :].astype(np.float32)
    cos_h, sin_h = np.cos(angles).astype(np.float32), np.sin(angles).astype(np.float32)
    return np.concatenate([cos_h, cos_h], axis=1), np.concatenate([-sin_h, sin_h], axis=1)


def solution(mesh):
    row_spec = P(('dp', 'ep'), None, None)
    vec_spec = P(None)
    mat_spec = P(None, None)
    cube_spec = P(None, None, None)
    expert_spec = P('ep', None, None)
    vmem = pl.BlockSpec(memory_space=pltpu.VMEM)
    hbm = pl.BlockSpec(memory_space=pl.ANY)

    def per_device(hidden, expert_ids, slot_ids, attn_norm, w_query, w_key, w_value, w_out, ffn_norm, ffn_gate, ffn_up, ffn_down, moe_norm, w_router, exp_gate, exp_up, exp_down):
        cos_t, sin_t = rope_tables()
        dma = pltpu.SemaphoreType.DMA
        call = pl.pallas_call(
            kernel,
            out_shape=pltpu.VMEM((TOK, DM), BF16),
            in_specs=[hbm] * 19,
            out_specs=vmem,
            scratch_shapes=[
                pltpu.VMEM((NSLOT, DM, CW), BF16),
                pltpu.VMEM((DEVS, NCB * TOK, CW), BF16),
                pltpu.VMEM((LOCAL, DEVS * CAP, DM), BF16),
                pltpu.VMEM((LOCAL, DEVS * CAP, EFF), BF16),
                pltpu.VMEM((NBW, 2, 4, HALF, BW), F32),
                pltpu.VMEM((2, 2, 4, HALF, BW), F32),
                pltpu.VMEM((4, 2, 4, HALF, BW), F32),
                pltpu.VMEM((NBW, 2, 2, HALF, BW), F32),
                pltpu.VMEM((NBW, 2, HALF, BW), F32),
                pltpu.VMEM((DEVS, 3 * TOK, ROWS), BF16),
                pltpu.VMEM((ROWS, TOK), BF16),
                pltpu.VMEM((DEVS, 2 * TOPK, TOK), F32),
                pltpu.VMEM((TOK, DM), BF16),
                pltpu.VMEM((2 * TOK, DM), BF16),
                pltpu.VMEM((NCB, TOK, CW), F32),
                pltpu.VMEM((NCB, TOK, CW), F32),
                pltpu.VMEM((TOK, DM), BF16),
                pltpu.VMEM((2 * TOK, FF // 2), BF16),
                pltpu.VMEM((2 * TOK, CW), F32),
                pltpu.VMEM((TOK, CW), BF16),
                pltpu.VMEM((TOK, CW), BF16),
                pltpu.VMEM((TOK, CW), BF16),
                dma((NSLOT,)), dma((1,)), dma((12,)), dma((1,)), dma((1,)),
                dma((2,)), dma((NBW, 2)), dma((1,)), dma((NBW,)), dma((1,)), dma((NBW,)),
                dma(()), dma(()), dma((1,)), dma((NCB,)), dma((9,)),
                pltpu.VMEM((TOK, DM), BF16),
                pltpu.VMEM((TOPK, TOK), jnp.int32),
                pltpu.VMEM((TOPK, TOK), jnp.int32),
                pltpu.VMEM((DM // LANE, LANE), BF16),
                pltpu.VMEM((DM // LANE, LANE), BF16),
                pltpu.VMEM((DM // LANE, LANE), BF16),
                pltpu.VMEM((NEXP, DM), BF16),
                pltpu.VMEM((TOK, HEAD), F32),
                pltpu.VMEM((TOK, HEAD), F32),
            ],
            compiler_params=pltpu.CompilerParams(collective_id=0, has_side_effects=True, vmem_limit_bytes=66000000),
            cost_estimate=pl.CostEstimate(flops=56_000_000_000, bytes_accessed=240_000_000, transcendentals=0),
        )
        res = call(
            hidden.reshape(TOK, DM), expert_ids.reshape(TOK, TOPK).T, slot_ids.reshape(TOK, TOPK).T,
            attn_norm.reshape(DM // LANE, LANE), ffn_norm.reshape(DM // LANE, LANE), moe_norm.reshape(DM // LANE, LANE), w_router.T, cos_t, sin_t,
            w_query, w_key, w_value, w_out.reshape(DM, DM), ffn_gate, ffn_up, ffn_down, exp_gate, exp_up, exp_down)
        return res.reshape(hidden.shape)

    return jax.shard_map(per_device, mesh=mesh, in_specs=(row_spec, row_spec, row_spec, vec_spec, mat_spec, mat_spec, mat_spec, cube_spec, vec_spec, mat_spec, mat_spec, mat_spec, vec_spec, mat_spec, expert_spec, expert_spec, expert_spec), out_specs=row_spec, check_vma=False)
```

```python
import functools

import jax
import jax.numpy as jnp
import numpy as np
from jax import lax
from jax.experimental import pallas as pl
from jax.experimental.pallas import tpu as pltpu
from jax.sharding import PartitionSpec as P

RMS_EPS = 1e-6
ROPE_BASE = 10000.0
F32 = jnp.float32
BF16 = jnp.bfloat16

DEVS = 8
TOK = 128
HALF = TOK // 2
DM = 2048
HEAD = 128
FF = 8192
LOCAL = 8
FOLD1_MID = ((5, 2),)
FOLD1_END = ((2, 0), (3, 1), (6, 3), (7, 4))
SEND2_START = ((3, 0), (4, 1), (7, 3))
EFF = 1024
TOPK = 8
LANE = 128
CAP = 48
ROWS = LOCAL * CAP
NEXP = DEVS * LOCAL
CW = 512
NCB = DM // CW
BW = 256
NBW = DM // BW
FF_PAIRS = FF // 2 // CW
NSLOT = 8
FF_EARLY = 2
FF_MID = 0

N_QKV = 12
N_OUT = 4
N_FFA = 2 * (FF_EARLY + FF_MID)
N_EGU = 4 * LOCAL
N_EDN = NBW * (LOCAL // 4)
N_LATE = FF_PAIRS - FF_EARLY - FF_MID
N_FFB = 2 * N_LATE
N_FK = FF // 2 // DM
N_FDN = NCB * N_FK
G_QKV = 0
G_OUT = G_QKV + N_QKV
G_FFA = G_OUT + N_OUT
G_EGU = G_FFA + N_FFA
G_EDN = G_EGU + N_EGU
G_FFB = G_EDN + N_EDN
G_FDN = G_FFB + N_FFB
G_END = G_FDN + N_FDN


def aligned(index, size):
    return pl.ds(pl.multiple_of(index * size, size), size)


def dot(lhs, rhs):
    return jnp.dot(lhs, rhs, preferred_element_type=F32)


def silu_mul(z_gate, z_up):
    return (jax.nn.silu(z_gate) * z_up).astype(BF16)


def kernel(hid_h, ids_h, slots_h, attn_norm_h, ffn_norm_h, moe_norm_h, w_router_h, cos_h, sin_h,
           w_query, w_key, w_value, w_out, ffn_gate, ffn_up, ffn_down, exp_gate, exp_up, exp_down,
           out,
           ring, toks, disp, hexp, pown, psib, recv0, recv1, recv2, gates, picks, route, ctx, xx, fsend, frecv, a_s, hff, facc, qs, ks, vs,
           ring_sem, ag_send, ag_recv, rt_send, rt_recv, s0_send, s0_recv, s1_send, s1_recv, s2_send, s2_recv, x_send, x_recv, f_send, f_recv, in_sem,
           hid, ids, slots, attn_norm, ffn_norm, moe_norm, w_router, cos_t, sin_t):
    me = lax.axis_index("ep")
    chip = me // 2
    core = me % 2
    sib = chip * 2 + 1 - core
    chip_x, chip_y, chip_d = chip + 1 - 2 * (chip % 2), (chip + 2) % 4, 3 - chip
    mine = aligned(core, TOK)
    src_x, src_y, src_d = chip_x * 2 + core, chip_y * 2 + core, chip_d * 2 + core

    def fetch(slot, src, part=None):
        dst = ring.at[slot] if part is None else ring.at[(slot,) + part]
        pltpu.make_async_copy(src, dst, ring_sem.at[slot]).start()

    def fetch_ffn(slot, pair, mat):
        fetch(slot, mat.at[:, aligned(core * FF_PAIRS + pair, CW)])

    def fetch_expert(slot, expert, col, mat):
        fetch(slot, mat.at[expert, :, aligned(col, CW)])

    def fetch_down(slot, col, quad):
        for i in range(4):
            fetch(slot, exp_down.at[quad * 4 + i, :, aligned(col, BW)], (pl.ds(i // 2 * EFF, EFF), pl.ds(i % 2 * BW, BW)))

    def fetch_ffn_down(slot, n, kk):
        fetch(slot, ffn_down.at[aligned(core * N_FK + kk, DM), aligned(n, CW)])

    def start(g, slot):
        def within(lo, hi):
            return pl.when(jnp.logical_and(g >= lo, g < hi))

        @within(G_QKV, G_OUT)
        def _():
            for which, mat in enumerate((w_query, w_key, w_value)):
                pl.when(g % 3 == which)(lambda mat=mat: fetch(slot, mat.at[:, aligned(g // 3, CW)]))

        @within(G_OUT, G_FFA)
        def _():
            fetch(slot, w_out.at[:, aligned(g - G_OUT, CW)])

        @within(G_FFA, G_EGU)
        def _():
            local = g - G_FFA
            for which, mat in enumerate((ffn_gate, ffn_up)):
                pl.when(local % 2 == which)(lambda mat=mat: fetch_ffn(slot, local // 2, mat))

        @within(G_EGU, G_EDN)
        def _():
            local = g - G_EGU
            for which, mat in enumerate((exp_gate, exp_up)):
                pl.when(local % 2 == which)(lambda mat=mat: fetch_expert(slot, local // 4, local // 2 % 2, mat))

    def start_now(g, slot):
        if g < G_OUT:
            fetch(slot, (w_query, w_key, w_value)[g % 3].at[:, pl.ds(g // 3 * CW, CW)])
        elif g < G_FFA:
            fetch(slot, w_out.at[:, pl.ds((g - G_OUT) * CW, CW)])
        elif g < G_EGU:
            fetch_ffn(slot, (g - G_FFA) // 2, (ffn_gate, ffn_up)[(g - G_FFA) % 2])
        else:
            local = g - G_EGU
            fetch_expert(slot, local // 4, local // 2 % 2, (exp_gate, exp_up)[local % 2])

    def ready(g):
        slot = g % NSLOT
        pltpu.make_async_copy(w_query.at[:, pl.ds(0, CW)], ring.at[slot], ring_sem.at[slot]).wait()
        return slot

    def done(g):
        start(g + NSLOT, g % NSLOT)

    def send(src, dst, send_sem, recv_sem, peer):
        return pltpu.make_async_remote_copy(src, dst, send_sem, recv_sem, device_id={"ep": peer}, device_id_type=pl.DeviceIdType.MESH)

    def ag_copy(src, cb, link, sem):
        block = toks.at[src, pl.ds(cb * TOK, TOK)]
        return send(block, block, ag_send.at[0], ag_recv.at[sem], (src_x, src_y, sib)[link])

    def ag_wait(blocks, sem):
        block = toks.at[0, pl.ds(0, blocks * TOK)]
        send(block, block, ag_send.at[0], ag_recv.at[sem], sib).wait_recv()

    def rt_copy(src, step):
        return send(route.at[src], route.at[src], rt_send.at[0], rt_recv.at[0], (me + step) % DEVS)

    first_dev, second_dev = (src_x, src_y), (src_y, src_x)
    slot_of = {"own": (0, 0), "x": (2, 1), "y": (1, 2), "d": (3, 3)}

    def s0_copy(b, half, late):
        part = pl.ds(0 if late else 2, 2)
        return send(psib.at[b % 2, half, part], recv0.at[b % 4, half, part], s0_send.at[b % 2], s0_recv.at[b, int(late)], sib)

    def s1_copy(b, half):
        return send(pown.at[b, half, pl.ds(2, 2)], recv1.at[b, half], s1_send.at[0], s1_recv.at[b], first_dev[half])

    def s2_copy(b, half):
        return send(pown.at[b, half, 1], recv2.at[b, half], s2_send.at[0], s2_recv.at[b], second_dev[half])

    def wait_sent(block, sem):
        send(block, block, sem, s2_recv.at[0], sib).wait_send()

    def wait_got(block, sem):
        send(block, block, s2_send.at[0], sem, sib).wait_recv()

    loads = {name: pltpu.make_async_copy(src, dst, in_sem.at[i]) for i, (name, src, dst) in enumerate((
        ("hid", hid_h, hid), ("moe_norm", moe_norm_h, moe_norm), ("attn_norm", attn_norm_h, attn_norm),
        ("w_router", w_router_h, w_router), ("ids", ids_h, ids), ("slots", slots_h, slots),
        ("cos", cos_h, cos_t), ("sin", sin_h, sin_t), ("ffn_norm", ffn_norm_h, ffn_norm)))}

    def loaded(*names):
        for name in names:
            loads[name].wait()

    barrier = pltpu.get_barrier_semaphore()
    for step in range(1, DEVS):
        pl.semaphore_signal(barrier, inc=1, device_id={"ep": (me + step) % DEVS}, device_id_type=pl.DeviceIdType.MESH)
    for load in loads.values():
        load.start()
    loaded("hid", "moe_norm", "attn_norm", "w_router", "ids", "slots", "cos", "sin", "ffn_norm")
    for g in range(NSLOT):
        start_now(g, g)

    hid_f = hid[...].astype(F32)
    inv_rms = lax.rsqrt(jnp.mean(hid_f * hid_f, axis=-1, keepdims=True) + RMS_EPS)
    for lt in range(DM // LANE):
        cols = slice(lt * LANE, (lt + 1) * LANE)
        cb, within_cb = divmod(lt * LANE, CW)
        part = hid[:, cols].astype(F32) * inv_rms
        toks[me, cb * TOK:(cb + 1) * TOK, within_cb:within_cb + LANE] = (part * moe_norm[lt:lt + 1, :].astype(F32)).astype(BF16)

    pl.semaphore_wait(barrier, DEVS - 1)
    for cb in range(NCB):
        ag_copy(me, cb, 0, min(cb, 2)).start()
        ag_copy(me, (cb + 2) % NCB, 1, 3 + min(cb, 2)).start()
        ag_copy(me, cb, 2, 8).start()

    for lt in range(DM // LANE):
        cols = slice(lt * LANE, (lt + 1) * LANE)
        xx[mine, cols] = (hid[:, cols].astype(F32) * inv_rms * attn_norm[lt:lt + 1, :].astype(F32)).astype(BF16)

    logits = jnp.zeros((NEXP, TOK), F32)
    for cb in range(NCB):
        logits = logits + lax.dot_general(w_router[:, cb * CW:(cb + 1) * CW], toks[me, cb * TOK:(cb + 1) * TOK, :], (((1,), (1,)), ((), ())), preferred_element_type=F32)
    expert_iota = lax.broadcasted_iota(jnp.int32, (NEXP, TOK), 0)
    chosen = jnp.concatenate([jnp.sum(jnp.where(expert_iota == ids[j:j + 1, :], logits, 0.0), axis=0, keepdims=True) for j in range(TOPK)], axis=0)
    raised = jnp.exp(chosen - jnp.max(chosen, axis=0, keepdims=True))
    route[me, 0:TOPK, :] = (ids[...] * CAP + slots[...]).astype(F32)
    route[me, TOPK:2 * TOPK, :] = raised / jnp.sum(raised, axis=0, keepdims=True)

    def relay(cb, sem_x, sem_y, sem_d):
        for src, block, link, sem, sem_sib in ((src_x, cb, 1, sem_x, 9), (src_y, cb + 2, 0, sem_y, 10)):
            ag_wait(1, sem)
            ag_copy(src, block, link, sem_d).start()
            ag_copy(src, block, 2, sem_sib).start()

    def forward(src, blocks, sem, sem_sib):
        ag_wait(2, sem)
        for cb in blocks:
            ag_copy(src, cb, 2, sem_sib).start()

    row_i = lax.broadcasted_iota(jnp.int32, (TOK, TOK), 0)
    col_i = lax.broadcasted_iota(jnp.int32, (TOK, TOK), 1)
    causal = row_i >= col_i

    def rope_into(dst, vals):
        for h in range(CW // HEAD):
            part = vals[:, h * HEAD:(h + 1) * HEAD]
            turned = part * cos_t[...] + pltpu.roll(part, HEAD // 2, 1) * sin_t[...]
            dst[:, h * HEAD:(h + 1) * HEAD] = turned.astype(BF16)

    def heads(hg):
        q, k, v = qs.at[hg % 2], ks.at[hg % 2], vs.at[hg % 2]
        for h in range(CW // HEAD):
            cols = slice(h * HEAD, (h + 1) * HEAD)
            scores = lax.dot_general(q[:, cols], k[:, cols], (((1,), (1,)), ((), ())), preferred_element_type=F32) * HEAD ** -0.5
            scores = jnp.where(causal, scores, -jnp.inf)
            expd = jnp.exp(scores - jnp.max(scores, axis=-1, keepdims=True))
            prob = (expd / jnp.sum(expd, axis=-1, keepdims=True)).astype(BF16)
            ctx[:, hg * CW + h * HEAD:hg * CW + (h + 1) * HEAD] = dot(prob, v[:, cols]).astype(BF16)

    for hg in range(NCB):
        g = G_QKV + hg * 3
        held = [ready(g + i) for i in range(3)]
        if hg:
            heads(hg - 1)
        rope_into(qs.at[hg % 2], dot(xx[mine], ring[held[0]]))
        rope_into(ks.at[hg % 2], dot(xx[mine], ring[held[1]]))
        vs[hg % 2] = dot(xx[mine], ring[held[2]]).astype(BF16)
        for i in range(3):
            start_now(g + i + NSLOT, held[i])
        if hg == 0:
            for step in range(1, DEVS):
                rt_copy(me, step).start()
        if hg == 2:
            relay(0, 0, 3, 6)

    def out_block(n, mixed):
        cols = slice(n * CW, (n + 1) * CW)
        a_s[:, cols] = (hid[:, cols].astype(F32) + mixed).astype(BF16)

    slot = ready(G_OUT)
    head_cols = (NCB - 1) * CW
    mixed = dot(ctx[:, 0:head_cols], ring[slot, 0:head_cols, :])
    heads(NCB - 1)
    out_block(0, mixed + dot(ctx[:, head_cols:DM], ring[slot, head_cols:DM, :]))
    start_now(G_OUT + NSLOT, slot)
    relay(1, 1, 4, 7)
    for n in range(1, N_OUT):
        slot = ready(G_OUT + n)
        out_block(n, dot(ctx[...], ring[slot]))
        start_now(G_OUT + n + NSLOT, slot)
    a_f = a_s[...].astype(F32)
    inv_rms = lax.rsqrt(jnp.mean(a_f * a_f, axis=-1, keepdims=True) + RMS_EPS)
    for lt in range(DM // LANE):
        cols = slice(lt * LANE, (lt + 1) * LANE)
        xx[aligned(core, TOK), cols] = (a_s[:, cols].astype(F32) * inv_rms * ffn_norm[lt:lt + 1, :].astype(F32)).astype(BF16)
    x_block = xx.at[aligned(core, TOK)]
    x_copy = send(x_block, x_block, x_send, x_recv, sib)

    def ffn_pair(g, col, refill, between=None):
        slot = ready(g)
        slot_up = ready(g + 1)
        if between is not None:
            between()
        z_gate = dot(xx[...], ring[slot])
        z_up = dot(xx[...], ring[slot_up])
        hff[:, aligned(col, CW)] = silu_mul(z_gate, z_up)
        refill(slot, slot_up)

    def ffn_early(i, carry):
        g = G_FFA + 2 * i

        def refill(slot, slot_up):
            done(g)
            done(g + 1)

        ffn_pair(g, i, refill)
        return carry

    def choose(src):
        want = lax.broadcasted_iota(jnp.int32, (ROWS, TOK), 0).astype(F32) + (me * ROWS).astype(F32)
        pick = jnp.zeros((ROWS, TOK), F32)
        gate = jnp.zeros((ROWS, TOK), F32)
        for j in range(TOPK):
            hit = route[src, j:j + 1, :] == want
            pick = jnp.where(hit, 1.0, pick)
            gate = jnp.where(hit, route[src, TOPK + j:TOPK + j + 1, :], gate)
        gate_t = jnp.transpose(gate)
        high = gate_t.astype(BF16)
        rest = gate_t - high.astype(F32)
        mid = rest.astype(BF16)
        low = (rest - mid.astype(F32)).astype(BF16)
        gates[src, 0:TOK, :] = high
        gates[src, TOK:2 * TOK, :] = mid
        gates[src, 2 * TOK:3 * TOK, :] = low
        picks[...] = pick.astype(BF16)

    def place(src):
        for cb in range(NCB):
            rows = dot(picks[...], toks[src, cb * TOK:(cb + 1) * TOK, :]).astype(BF16)
            for e in range(LOCAL):
                disp[e, pl.ds(pl.multiple_of(src * CAP, 16), CAP), cb * CW:(cb + 1) * CW] = rows[e * CAP:(e + 1) * CAP, :]

    def dispatch(src, carry):
        choose(src)
        place(src)
        return carry

    def dispatch_two(one, two):
        lax.fori_loop(0, 2, lambda i, carry: dispatch(one + i * (two - one), carry), 0)

    wait_got(route.at[pl.ds(0, DEVS - 1)], rt_recv.at[0])
    ag_wait(4, 8)
    x_copy.start()
    dispatch_two(me, sib)
    forward(src_x, (2, 3), 2, 9)
    forward(src_y, (0, 1), 5, 10)
    dispatch_two(src_x, src_y)
    x_copy.wait()
    lax.fori_loop(0, FF_EARLY, ffn_early, 0)
    sib_x, sib_y, sib_d = (c * 2 + 1 - core for c in (chip_x, chip_y, chip_d))
    ag_wait(4, 9)
    ag_wait(4, 10)
    forward(src_d, (0, 2), 6, 11)
    dispatch(sib_x, 0)
    forward(src_d, (1, 3), 7, 11)
    dispatch(sib_y, 0)
    lax.fori_loop(FF_EARLY, FF_EARLY + FF_MID, ffn_early, 0)
    dispatch(src_d, 0)
    choose(sib_d)
    ag_wait(4, 11)
    place(sib_d)

    wait_sent(toks.at[pl.ds(0, 7)], ag_send.at[0])
    wait_sent(route.at[pl.ds(0, DEVS - 1)], rt_send.at[0])

    def expert_up(expert, carry):
        g = G_EGU + 4 * expert
        held = [ready(g + i) for i in range(4)]
        for quarter in range(2):
            z_gate = dot(disp[expert], ring[held[quarter * 2]])
            z_up = dot(disp[expert], ring[held[quarter * 2 + 1]])
            hexp[expert, :, quarter * 512:(quarter + 1) * 512] = silu_mul(z_gate, z_up)

        @pl.when(expert < LOCAL - 2)
        def _():
            for i in range(4):
                fetch_expert(held[i], expert + 2, i // 2, (exp_gate, exp_up)[i % 2])

        @pl.when(expert >= LOCAL - 2)
        def _():
            for i in range(4):
                fetch_down(held[i], (expert - (LOCAL - 2)) * 2 + i // 2, i % 2)
        return carry

    lax.fori_loop(0, LOCAL, expert_up, 0)

    def fold0(b, late):
        wait_got(recv0.at[0, 0], s0_recv.at[b, int(late)])
        for half in range(2):
            part = slice(0, 2) if late else slice(2, 4)
            pown[b, half, part] = pown[b, half, part] + recv0[b % 4, half, part]

    def start0(b, late):
        for half in range(2):
            s0_copy(b, half, late).start()

    def send1(b):
        for half in range(2):
            s1_copy(b, half).start()

    def fold1(b):
        wait_got(recv1.at[b], s1_recv.at[b])
        for half in range(2):
            pown[b, half, 0:2] = pown[b, half, 0:2] + recv1[b, half]

    def send2(b):
        for half in range(2):
            s2_copy(b, half).start()

    def down_block(b, carry):
        def down_quad(quad, slot):
            for i in range(4):
                e = quad * 4 + i
                y = dot(hexp[e], ring[slot, i // 2 * EFF:(i // 2 + 1) * EFF, i % 2 * BW:(i % 2 + 1) * BW]).astype(BF16)
                for s in range(DEVS):
                    toks[s, e * CAP:(e + 1) * CAP, 0:BW] = y[s * CAP:(s + 1) * CAP, :]
            pl.when(b < NBW - 4)(lambda: fetch_down(slot, b + 4, quad))
            pl.when(b >= NBW - 4)(lambda: fetch_ffn(slot, FF_EARLY + FF_MID + b - (NBW - 4), (ffn_gate, ffn_up)[quad]))

        def at(table, act):
            for step, block in table:
                pl.when(b == step)(functools.partial(act, block))

        def combine(dest, side):
            for name, c in (("d", chip_d), ("x", chip_x), ("y", chip_y), ("own", chip)):
                parts = dot(gates[c * 2 + side], toks[c * 2 + side, 0:ROWS, 0:BW])
                moe = parts[0:TOK] + parts[TOK:2 * TOK] + parts[2 * TOK:3 * TOK]
                for half in range(2):
                    dest[half, slot_of[name][half]] = moe[half * HALF:(half + 1) * HALF]

        g = G_EDN + b * 2
        slot = ready(g)
        at(SEND2_START, send2)
        down_quad(0, slot)

        @pl.when(b >= 1)
        def _():
            fold0(b - 1, False)

        at(FOLD1_MID, fold1)

        @pl.when(b >= 2)
        def _():
            wait_sent(psib.at[b % 2], s0_send.at[b % 2])

        slot = ready(g + 1)
        pl.when(b >= 1)(lambda: send1(b - 1))
        at(FOLD1_MID, send2)
        down_quad(1, slot)
        pl.when(b >= 1)(lambda: fold0(b - 1, True))
        combine(psib.at[b % 2], 1 - core)
        start0(b, False)
        combine(pown.at[b], core)
        start0(b, True)
        at(FOLD1_END, fold1)
        return carry

    lax.fori_loop(0, NBW, down_block, 0)

    def ffn_late(i, carry):
        g = G_FFB + 2 * i

        def refill(slot, slot_up):
            pair = i + 4

            @pl.when(pair < N_LATE)
            def _():
                fetch_ffn(slot, FF_EARLY + FF_MID + pair, ffn_gate)
                fetch_ffn(slot_up, FF_EARLY + FF_MID + pair, ffn_up)

            @pl.when(pair >= N_LATE)
            def _():
                fetch_ffn_down(slot, pair - N_LATE, 0)
                fetch_ffn_down(slot_up, pair - N_LATE, 1)

        def before():
            for step, act in ((0, lambda: send2(4)), (1, lambda: send1(NBW - 1)), (2, lambda: send2(5)), (5, lambda: send2(6))):
                pl.when(i == step)(act)

        ffn_pair(g, FF_EARLY + FF_MID + i, refill, before)
        for step, act in ((0, lambda: fold0(NBW - 1, False)), (1, lambda: fold0(NBW - 1, True)), (1, lambda: fold1(5)), (4, lambda: fold1(6))):
            pl.when(i == step)(act)
        return carry

    lax.fori_loop(0, N_LATE, ffn_late, 0)

    def f_copy(n):
        return send(fsend.at[n], frecv.at[n], f_send.at[0], f_recv.at[n], sib)

    def ffn_out(n, carry):
        g = G_FDN + n * N_FK
        held = [ready(g + kk) for kk in range(N_FK)]
        pl.when(n == 2)(lambda: send2(NBW - 1))
        facc[...] = sum(dot(hff[:, kk * DM:(kk + 1) * DM], ring[held[kk]]) for kk in range(N_FK))
        fsend[n] = facc[aligned(1 - core, TOK), :]
        for w in range(CW // BW):
            b = n * (CW // BW) + w
            for half in range(2):
                own = facc[pl.ds(pl.multiple_of(core * TOK + half * HALF, HALF), HALF), w * BW:(w + 1) * BW]
                pown[b, half, 0] = pown[b, half, 0] + own
        pl.when(n >= 1)(lambda: f_copy(n - 1).start())
        pl.when(n == 1)(lambda: fold1(NBW - 1))
        return carry

    lax.fori_loop(0, NCB, ffn_out, 0)

    def final(n):
        f_copy(n).wait_recv()
        for w in range(CW // BW):
            b = n * (CW // BW) + w
            cols = slice(b * BW, (b + 1) * BW)
            wait_got(recv2.at[b], s2_recv.at[b])
            for half in range(2):
                rows = slice(half * HALF, (half + 1) * HALF)
                total = pown[b, half, 0] + recv2[b, half] + frecv[n, rows, w * BW:(w + 1) * BW]
                out[rows, cols] = (a_s[rows, cols].astype(F32) + total).astype(BF16)

    final(0)
    f_copy(NCB - 1).start()
    final(1)
    final(2)
    wait_sent(pown.at[pl.ds(0, 4)], s1_send.at[0])
    for parity in range(2):
        wait_sent(psib.at[parity], s0_send.at[parity])
    wait_sent(fsend, f_send.at[0])
    final(3)
    wait_sent(pown.at[pl.ds(0, 2)], s2_send.at[0])


def rope_tables():
    half = HEAD // 2
    inv_freq = np.float32(ROPE_BASE) ** (np.float32(-2.0) * np.arange(half, dtype=np.float32) / np.float32(HEAD))
    angles = np.arange(TOK, dtype=np.float32)[:, None] * inv_freq[None, :].astype(np.float32)
    cos_h, sin_h = np.cos(angles).astype(np.float32), np.sin(angles).astype(np.float32)
    return np.concatenate([cos_h, cos_h], axis=1), np.concatenate([-sin_h, sin_h], axis=1)


def solution(mesh):
    row_spec = P(('dp', 'ep'), None, None)
    vec_spec = P(None)
    mat_spec = P(None, None)
    cube_spec = P(None, None, None)
    expert_spec = P('ep', None, None)
    vmem = pl.BlockSpec(memory_space=pltpu.VMEM)
    hbm = pl.BlockSpec(memory_space=pl.ANY)

    def per_device(hidden, expert_ids, slot_ids, attn_norm, w_query, w_key, w_value, w_out, ffn_norm, ffn_gate, ffn_up, ffn_down, moe_norm, w_router, exp_gate, exp_up, exp_down):
        cos_t, sin_t = rope_tables()
        dma = pltpu.SemaphoreType.DMA
        call = pl.pallas_call(
            kernel,
            out_shape=pltpu.VMEM((TOK, DM), BF16),
            in_specs=[hbm] * 19,
            out_specs=vmem,
            scratch_shapes=[
                pltpu.VMEM((NSLOT, DM, CW), BF16),
                pltpu.VMEM((DEVS, NCB * TOK, CW), BF16),
                pltpu.VMEM((LOCAL, DEVS * CAP, DM), BF16),
                pltpu.VMEM((LOCAL, DEVS * CAP, EFF), BF16),
                pltpu.VMEM((NBW, 2, 4, HALF, BW), F32),
                pltpu.VMEM((2, 2, 4, HALF, BW), F32),
                pltpu.VMEM((4, 2, 4, HALF, BW), F32),
                pltpu.VMEM((NBW, 2, 2, HALF, BW), F32),
                pltpu.VMEM((NBW, 2, HALF, BW), F32),
                pltpu.VMEM((DEVS, 3 * TOK, ROWS), BF16),
                pltpu.VMEM((ROWS, TOK), BF16),
                pltpu.VMEM((DEVS, 2 * TOPK, TOK), F32),
                pltpu.VMEM((TOK, DM), BF16),
                pltpu.VMEM((2 * TOK, DM), BF16),
                pltpu.VMEM((NCB, TOK, CW), F32),
                pltpu.VMEM((NCB, TOK, CW), F32),
                pltpu.VMEM((TOK, DM), BF16),
                pltpu.VMEM((2 * TOK, FF // 2), BF16),
                pltpu.VMEM((2 * TOK, CW), F32),
                pltpu.VMEM((2, TOK, CW), BF16),
                pltpu.VMEM((2, TOK, CW), BF16),
                pltpu.VMEM((2, TOK, CW), BF16),
                dma((NSLOT,)), dma((1,)), dma((12,)), dma((1,)), dma((1,)),
                dma((2,)), dma((NBW, 2)), dma((1,)), dma((NBW,)), dma((1,)), dma((NBW,)),
                dma(()), dma(()), dma((1,)), dma((NCB,)), dma((9,)),
                pltpu.VMEM((TOK, DM), BF16),
                pltpu.VMEM((TOPK, TOK), jnp.int32),
                pltpu.VMEM((TOPK, TOK), jnp.int32),
                pltpu.VMEM((DM // LANE, LANE), BF16),
                pltpu.VMEM((DM // LANE, LANE), BF16),
                pltpu.VMEM((DM // LANE, LANE), BF16),
                pltpu.VMEM((NEXP, DM), BF16),
                pltpu.VMEM((TOK, HEAD), F32),
                pltpu.VMEM((TOK, HEAD), F32),
            ],
            compiler_params=pltpu.CompilerParams(collective_id=0, has_side_effects=True, vmem_limit_bytes=66000000),
            cost_estimate=pl.CostEstimate(flops=56_000_000_000, bytes_accessed=240_000_000, transcendentals=0),
        )
        res = call(
            hidden.reshape(TOK, DM), expert_ids.reshape(TOK, TOPK).T, slot_ids.reshape(TOK, TOPK).T,
            attn_norm.reshape(DM // LANE, LANE), ffn_norm.reshape(DM // LANE, LANE), moe_norm.reshape(DM // LANE, LANE), w_router.T, cos_t, sin_t,
            w_query, w_key, w_value, w_out.reshape(DM, DM), ffn_gate, ffn_up, ffn_down, exp_gate, exp_up, exp_down)
        return res.reshape(hidden.shape)

    return jax.shard_map(per_device, mesh=mesh, in_specs=(row_spec, row_spec, row_spec, vec_spec, mat_spec, mat_spec, mat_spec, cube_spec, vec_spec, mat_spec, mat_spec, mat_spec, vec_spec, mat_spec, expert_spec, expert_spec, expert_spec), out_specs=row_spec, check_vma=False)
```

```python
import functools

import jax
import jax.numpy as jnp
import numpy as np
from jax import lax
from jax.experimental import pallas as pl
from jax.experimental.pallas import tpu as pltpu
from jax.sharding import PartitionSpec as P

RMS_EPS = 1e-6
ROPE_BASE = 10000.0
F32 = jnp.float32
BF16 = jnp.bfloat16

DEVS = 8
TOK = 128
HALF = TOK // 2
DM = 2048
HEAD = 128
FF = 8192
LOCAL = 8
FOLD1_MID = ((5, 2),)
FOLD1_END = ((2, 0), (3, 1), (6, 3), (7, 4))
SEND2_START = ((3, 0), (4, 1), (7, 3))
EFF = 1024
TOPK = 8
LANE = 128
CAP = 48
ROWS = LOCAL * CAP
NEXP = DEVS * LOCAL
CW = 512
NCB = DM // CW
BW = 256
NBW = DM // BW
FF_PAIRS = FF // 2 // CW
NSLOT = 8
FF_EARLY = 2
FF_MID = 0

N_QKV = 12
N_OUT = 4
N_FFA = 2 * (FF_EARLY + FF_MID)
N_EGU = 4 * LOCAL
N_EDN = NBW * (LOCAL // 4)
N_LATE = FF_PAIRS - FF_EARLY - FF_MID
N_FFB = 2 * N_LATE
N_FK = FF // 2 // DM
N_FDN = NCB * N_FK
G_QKV = 0
G_OUT = G_QKV + N_QKV
G_FFA = G_OUT + N_OUT
G_EGU = G_FFA + N_FFA
G_EDN = G_EGU + N_EGU
G_FFB = G_EDN + N_EDN
G_FDN = G_FFB + N_FFB
G_END = G_FDN + N_FDN


def aligned(index, size):
    return pl.ds(pl.multiple_of(index * size, size), size)


def dot(lhs, rhs):
    return jnp.dot(lhs, rhs, preferred_element_type=F32)


def silu_mul(z_gate, z_up):
    return (jax.nn.silu(z_gate) * z_up).astype(BF16)


def kernel(hid_h, ids_h, slots_h, attn_norm_h, ffn_norm_h, moe_norm_h, w_router_h, cos_h, sin_h,
           w_query, w_key, w_value, w_out, ffn_gate, ffn_up, ffn_down, exp_gate, exp_up, exp_down,
           out,
           ring, toks, disp, hexp, pown, psib, recv0, recv1, recv2, gates, picks, route, ctx, xx, fsend, frecv, a_s, hff, facc, qs, ks, vs,
           ring_sem, ag_send, ag_recv, rt_send, rt_recv, s0_send, s0_recv, s1_send, s1_recv, s2_send, s2_recv, x_send, x_recv, f_send, f_recv, in_sem,
           hid, ids, slots, attn_norm, ffn_norm, moe_norm, w_router, cos_t, sin_t):
    me = lax.axis_index("ep")
    chip = me // 2
    core = me % 2
    sib = chip * 2 + 1 - core
    chip_x, chip_y, chip_d = chip + 1 - 2 * (chip % 2), (chip + 2) % 4, 3 - chip
    mine = aligned(core, TOK)
    src_x, src_y, src_d = chip_x * 2 + core, chip_y * 2 + core, chip_d * 2 + core

    def fetch(slot, src, part=None):
        dst = ring.at[slot] if part is None else ring.at[(slot,) + part]
        pltpu.make_async_copy(src, dst, ring_sem.at[slot]).start()

    def fetch_ffn(slot, pair, mat):
        fetch(slot, mat.at[:, aligned(core * FF_PAIRS + pair, CW)])

    def fetch_expert(slot, expert, col, mat):
        fetch(slot, mat.at[expert, :, aligned(col, CW)])

    def fetch_down(slot, col, quad):
        for i in range(4):
            fetch(slot, exp_down.at[quad * 4 + i, :, aligned(col, BW)], (pl.ds(i // 2 * EFF, EFF), pl.ds(i % 2 * BW, BW)))

    def fetch_ffn_down(slot, n, kk):
        fetch(slot, ffn_down.at[aligned(core * N_FK + kk, DM), aligned(n, CW)])

    def start(g, slot):
        def within(lo, hi):
            return pl.when(jnp.logical_and(g >= lo, g < hi))

        @within(G_QKV, G_OUT)
        def _():
            for which, mat in enumerate((w_query, w_key, w_value)):
                pl.when(g % 3 == which)(lambda mat=mat: fetch(slot, mat.at[:, aligned(g // 3, CW)]))

        @within(G_OUT, G_FFA)
        def _():
            fetch(slot, w_out.at[:, aligned(g - G_OUT, CW)])

        @within(G_FFA, G_EGU)
        def _():
            local = g - G_FFA
            for which, mat in enumerate((ffn_gate, ffn_up)):
                pl.when(local % 2 == which)(lambda mat=mat: fetch_ffn(slot, local // 2, mat))

        @within(G_EGU, G_EDN)
        def _():
            local = g - G_EGU
            for which, mat in enumerate((exp_gate, exp_up)):
                pl.when(local % 2 == which)(lambda mat=mat: fetch_expert(slot, local // 4, local // 2 % 2, mat))

    def start_now(g, slot):
        if g < G_OUT:
            fetch(slot, (w_query, w_key, w_value)[g % 3].at[:, pl.ds(g // 3 * CW, CW)])
        elif g < G_FFA:
            fetch(slot, w_out.at[:, pl.ds((g - G_OUT) * CW, CW)])
        elif g < G_EGU:
            fetch_ffn(slot, (g - G_FFA) // 2, (ffn_gate, ffn_up)[(g - G_FFA) % 2])
        else:
            local = g - G_EGU
            fetch_expert(slot, local // 4, local // 2 % 2, (exp_gate, exp_up)[local % 2])

    def ready(g):
        slot = g % NSLOT
        pltpu.make_async_copy(w_query.at[:, pl.ds(0, CW)], ring.at[slot], ring_sem.at[slot]).wait()
        return slot

    def done(g):
        start(g + NSLOT, g % NSLOT)

    def send(src, dst, send_sem, recv_sem, peer):
        return pltpu.make_async_remote_copy(src, dst, send_sem, recv_sem, device_id={"ep": peer}, device_id_type=pl.DeviceIdType.MESH)

    def ag_copy(src, cb, link, sem):
        block = toks.at[src, pl.ds(cb * TOK, TOK)]
        return send(block, block, ag_send.at[0], ag_recv.at[sem], (src_x, src_y, sib)[link])

    def ag_wait(blocks, sem):
        block = toks.at[0, pl.ds(0, blocks * TOK)]
        send(block, block, ag_send.at[0], ag_recv.at[sem], sib).wait_recv()

    def rt_copy(src, step):
        return send(route.at[src], route.at[src], rt_send.at[0], rt_recv.at[0], (me + step) % DEVS)

    first_dev, second_dev = (src_x, src_y), (src_y, src_x)
    slot_of = {"own": (0, 0), "x": (2, 1), "y": (1, 2), "d": (3, 3)}

    def s0_copy(b, half, late):
        part = pl.ds(0 if late else 2, 2)
        return send(psib.at[b % 2, half, part], recv0.at[b % 4, half, part], s0_send.at[b % 2], s0_recv.at[b, int(late)], sib)

    def s1_copy(b, half):
        return send(pown.at[b, half, pl.ds(2, 2)], recv1.at[b, half], s1_send.at[0], s1_recv.at[b], first_dev[half])

    def s2_copy(b, half):
        return send(pown.at[b, half, 1], recv2.at[b, half], s2_send.at[0], s2_recv.at[b], second_dev[half])

    def wait_sent(block, sem):
        send(block, block, sem, s2_recv.at[0], sib).wait_send()

    def wait_got(block, sem):
        send(block, block, s2_send.at[0], sem, sib).wait_recv()

    loads = {name: pltpu.make_async_copy(src, dst, in_sem.at[i]) for i, (name, src, dst) in enumerate((
        ("hid", hid_h, hid), ("moe_norm", moe_norm_h, moe_norm), ("attn_norm", attn_norm_h, attn_norm),
        ("w_router", w_router_h, w_router), ("ids", ids_h, ids), ("slots", slots_h, slots),
        ("cos", cos_h, cos_t), ("sin", sin_h, sin_t), ("ffn_norm", ffn_norm_h, ffn_norm)))}

    def loaded(*names):
        for name in names:
            loads[name].wait()

    barrier = pltpu.get_barrier_semaphore()
    for step in range(1, DEVS):
        pl.semaphore_signal(barrier, inc=1, device_id={"ep": (me + step) % DEVS}, device_id_type=pl.DeviceIdType.MESH)
    for load in loads.values():
        load.start()
    loaded("hid", "moe_norm", "attn_norm", "w_router", "ids", "slots", "cos", "sin", "ffn_norm")
    for g in range(NSLOT):
        start_now(g, g)

    hid_f = hid[...].astype(F32)
    inv_rms = lax.rsqrt(jnp.mean(hid_f * hid_f, axis=-1, keepdims=True) + RMS_EPS)
    for lt in range(DM // LANE):
        cols = slice(lt * LANE, (lt + 1) * LANE)
        cb, within_cb = divmod(lt * LANE, CW)
        part = hid[:, cols].astype(F32) * inv_rms
        toks[me, cb * TOK:(cb + 1) * TOK, within_cb:within_cb + LANE] = (part * moe_norm[lt:lt + 1, :].astype(F32)).astype(BF16)

    pl.semaphore_wait(barrier, DEVS - 1)
    for cb in range(NCB):
        ag_copy(me, cb, 0, min(cb, 2)).start()
        ag_copy(me, (cb + 2) % NCB, 1, 3 + min(cb, 2)).start()
        ag_copy(me, cb, 2, 8).start()

    for lt in range(DM // LANE):
        cols = slice(lt * LANE, (lt + 1) * LANE)
        xx[mine, cols] = (hid[:, cols].astype(F32) * inv_rms * attn_norm[lt:lt + 1, :].astype(F32)).astype(BF16)

    logits = jnp.zeros((NEXP, TOK), F32)
    for cb in range(NCB):
        logits = logits + lax.dot_general(w_router[:, cb * CW:(cb + 1) * CW], toks[me, cb * TOK:(cb + 1) * TOK, :], (((1,), (1,)), ((), ())), preferred_element_type=F32)
    expert_iota = lax.broadcasted_iota(jnp.int32, (NEXP, TOK), 0)
    chosen = jnp.concatenate([jnp.sum(jnp.where(expert_iota == ids[j:j + 1, :], logits, 0.0), axis=0, keepdims=True) for j in range(TOPK)], axis=0)
    raised = jnp.exp(chosen - jnp.max(chosen, axis=0, keepdims=True))
    route[me, 0:TOPK, :] = (ids[...] * CAP + slots[...]).astype(F32)
    route[me, TOPK:2 * TOPK, :] = raised / jnp.sum(raised, axis=0, keepdims=True)

    def relay(cb, sem_x, sem_y, sem_d):
        for src, block, link, sem, sem_sib in ((src_x, cb, 1, sem_x, 9), (src_y, cb + 2, 0, sem_y, 10)):
            ag_wait(1, sem)
            ag_copy(src, block, link, sem_d).start()
            ag_copy(src, block, 2, sem_sib).start()

    def forward(src, blocks, sem, sem_sib):
        ag_wait(2, sem)
        for cb in blocks:
            ag_copy(src, cb, 2, sem_sib).start()

    row_i = lax.broadcasted_iota(jnp.int32, (TOK, TOK), 0)
    col_i = lax.broadcasted_iota(jnp.int32, (TOK, TOK), 1)
    causal = row_i >= col_i

    def rope_into(dst, vals):
        for h in range(CW // HEAD):
            part = vals[:, h * HEAD:(h + 1) * HEAD]
            turned = part * cos_t[...] + pltpu.roll(part, HEAD // 2, 1) * sin_t[...]
            dst[:, h * HEAD:(h + 1) * HEAD] = turned.astype(BF16)

    def heads(hg):
        q, k, v = qs.at[hg % 2], ks.at[hg % 2], vs.at[hg % 2]
        for h in range(CW // HEAD):
            cols = slice(h * HEAD, (h + 1) * HEAD)
            scores = lax.dot_general(q[:, cols], k[:, cols], (((1,), (1,)), ((), ())), preferred_element_type=F32) * HEAD ** -0.5
            scores = jnp.where(causal, scores, -jnp.inf)
            expd = jnp.exp(scores - jnp.max(scores, axis=-1, keepdims=True))
            prob = (expd / jnp.sum(expd, axis=-1, keepdims=True)).astype(BF16)
            ctx[:, hg * CW + h * HEAD:hg * CW + (h + 1) * HEAD] = dot(prob, v[:, cols]).astype(BF16)

    for hg in range(NCB):
        g = G_QKV + hg * 3
        held = [ready(g + i) for i in range(3)]
        if hg:
            heads(hg - 1)
        rope_into(qs.at[hg % 2], dot(xx[mine], ring[held[0]]))
        rope_into(ks.at[hg % 2], dot(xx[mine], ring[held[1]]))
        vs[hg % 2] = dot(xx[mine], ring[held[2]]).astype(BF16)
        for i in range(3):
            start_now(g + i + NSLOT, held[i])
        if hg == 0:
            for step in range(1, DEVS):
                rt_copy(me, step).start()
        if hg == 2:
            relay(0, 0, 3, 6)

    def out_block(n, mixed):
        cols = slice(n * CW, (n + 1) * CW)
        a_s[:, cols] = (hid[:, cols].astype(F32) + mixed).astype(BF16)

    slot = ready(G_OUT)
    head_cols = (NCB - 1) * CW
    mixed = dot(ctx[:, 0:head_cols], ring[slot, 0:head_cols, :])
    heads(NCB - 1)
    out_block(0, mixed + dot(ctx[:, head_cols:DM], ring[slot, head_cols:DM, :]))
    start_now(G_OUT + NSLOT, slot)
    relay(1, 1, 4, 7)
    for n in range(1, N_OUT):
        slot = ready(G_OUT + n)
        out_block(n, dot(ctx[...], ring[slot]))
        start_now(G_OUT + n + NSLOT, slot)
    a_f = a_s[...].astype(F32)
    inv_rms = lax.rsqrt(jnp.mean(a_f * a_f, axis=-1, keepdims=True) + RMS_EPS)
    for lt in range(DM // LANE):
        cols = slice(lt * LANE, (lt + 1) * LANE)
        xx[aligned(core, TOK), cols] = (a_s[:, cols].astype(F32) * inv_rms * ffn_norm[lt:lt + 1, :].astype(F32)).astype(BF16)
    x_block = xx.at[aligned(core, TOK)]
    x_copy = send(x_block, x_block, x_send, x_recv, sib)

    def ffn_pair(g, col, refill, between=None):
        slot = ready(g)
        slot_up = ready(g + 1)
        if between is not None:
            between()
        z_gate = dot(xx[...], ring[slot])
        z_up = dot(xx[...], ring[slot_up])
        hff[:, aligned(col, CW)] = silu_mul(z_gate, z_up)
        refill(slot, slot_up)

    def ffn_early(i, carry):
        g = G_FFA + 2 * i

        def refill(slot, slot_up):
            done(g)
            done(g + 1)

        ffn_pair(g, i, refill)
        return carry

    def wanted_rows():
        return lax.broadcasted_iota(jnp.int32, (ROWS, TOK), 0).astype(F32) + (me * ROWS).astype(F32)

    def choose(src):
        want = wanted_rows()
        pick = jnp.zeros((ROWS, TOK), F32)
        for j in range(TOPK):
            pick = jnp.where(route[src, j:j + 1, :] == want, 1.0, pick)
        picks[...] = pick.astype(BF16)

    def weigh(src):
        want = wanted_rows()
        gate = jnp.zeros((ROWS, TOK), F32)
        for j in range(TOPK):
            gate = jnp.where(route[src, j:j + 1, :] == want, route[src, TOPK + j:TOPK + j + 1, :], gate)
        gate_t = jnp.transpose(gate)
        high = gate_t.astype(BF16)
        rest = gate_t - high.astype(F32)
        mid = rest.astype(BF16)
        low = (rest - mid.astype(F32)).astype(BF16)
        gates[src, 0:TOK, :] = high
        gates[src, TOK:2 * TOK, :] = mid
        gates[src, 2 * TOK:3 * TOK, :] = low

    def place(src):
        for cb in range(NCB):
            rows = dot(picks[...], toks[src, cb * TOK:(cb + 1) * TOK, :]).astype(BF16)
            for e in range(LOCAL):
                disp[e, pl.ds(pl.multiple_of(src * CAP, 16), CAP), cb * CW:(cb + 1) * CW] = rows[e * CAP:(e + 1) * CAP, :]

    def dispatch(src, carry):
        choose(src)
        place(src)
        return carry

    def dispatch_two(one, two):
        lax.fori_loop(0, 2, lambda i, carry: dispatch(one + i * (two - one), carry), 0)

    wait_got(route.at[pl.ds(0, DEVS - 1)], rt_recv.at[0])
    ag_wait(4, 8)
    x_copy.start()
    dispatch_two(me, sib)
    forward(src_x, (2, 3), 2, 9)
    forward(src_y, (0, 1), 5, 10)
    dispatch_two(src_x, src_y)
    x_copy.wait()
    lax.fori_loop(0, FF_EARLY, ffn_early, 0)
    sib_x, sib_y, sib_d = (c * 2 + 1 - core for c in (chip_x, chip_y, chip_d))
    ag_wait(4, 9)
    ag_wait(4, 10)
    forward(src_d, (0, 2), 6, 11)
    dispatch(sib_x, 0)
    forward(src_d, (1, 3), 7, 11)
    dispatch(sib_y, 0)
    lax.fori_loop(FF_EARLY, FF_EARLY + FF_MID, ffn_early, 0)
    dispatch(src_d, 0)
    choose(sib_d)
    ag_wait(4, 11)
    place(sib_d)

    wait_sent(toks.at[pl.ds(0, 7)], ag_send.at[0])
    wait_sent(route.at[pl.ds(0, DEVS - 1)], rt_send.at[0])

    def expert_up(expert, carry):
        g = G_EGU + 4 * expert
        held = [ready(g + i) for i in range(4)]
        weigh(expert)
        for quarter in range(2):
            z_gate = dot(disp[expert], ring[held[quarter * 2]])
            z_up = dot(disp[expert], ring[held[quarter * 2 + 1]])
            hexp[expert, :, quarter * 512:(quarter + 1) * 512] = silu_mul(z_gate, z_up)

        @pl.when(expert < LOCAL - 2)
        def _():
            for i in range(4):
                fetch_expert(held[i], expert + 2, i // 2, (exp_gate, exp_up)[i % 2])

        @pl.when(expert >= LOCAL - 2)
        def _():
            for i in range(4):
                fetch_down(held[i], (expert - (LOCAL - 2)) * 2 + i // 2, i % 2)
        return carry

    lax.fori_loop(0, LOCAL, expert_up, 0)

    def fold0(b, late):
        wait_got(recv0.at[0, 0], s0_recv.at[b, int(late)])
        for half in range(2):
            part = slice(0, 2) if late else slice(2, 4)
            pown[b, half, part] = pown[b, half, part] + recv0[b % 4, half, part]

    def start0(b, late):
        for half in range(2):
            s0_copy(b, half, late).start()

    def send1(b):
        for half in range(2):
            s1_copy(b, half).start()

    def fold1(b):
        wait_got(recv1.at[b], s1_recv.at[b])
        for half in range(2):
            pown[b, half, 0:2] = pown[b, half, 0:2] + recv1[b, half]

    def send2(b):
        for half in range(2):
            s2_copy(b, half).start()

    def down_block(b, carry):
        def down_quad(quad, slot):
            for i in range(4):
                e = quad * 4 + i
                y = dot(hexp[e], ring[slot, i // 2 * EFF:(i // 2 + 1) * EFF, i % 2 * BW:(i % 2 + 1) * BW]).astype(BF16)
                for s in range(DEVS):
                    toks[s, e * CAP:(e + 1) * CAP, 0:BW] = y[s * CAP:(s + 1) * CAP, :]
            pl.when(b < NBW - 4)(lambda: fetch_down(slot, b + 4, quad))
            pl.when(b >= NBW - 4)(lambda: fetch_ffn(slot, FF_EARLY + FF_MID + b - (NBW - 4), (ffn_gate, ffn_up)[quad]))

        def at(table, act):
            for step, block in table:
                pl.when(b == step)(functools.partial(act, block))

        def combine(dest, side):
            for name, c in (("d", chip_d), ("x", chip_x), ("y", chip_y), ("own", chip)):
                parts = dot(gates[c * 2 + side], toks[c * 2 + side, 0:ROWS, 0:BW])
                moe = parts[0:TOK] + parts[TOK:2 * TOK] + parts[2 * TOK:3 * TOK]
                for half in range(2):
                    dest[half, slot_of[name][half]] = moe[half * HALF:(half + 1) * HALF]

        g = G_EDN + b * 2
        slot = ready(g)
        at(SEND2_START, send2)
        down_quad(0, slot)

        @pl.when(b >= 1)
        def _():
            fold0(b - 1, False)

        at(FOLD1_MID, fold1)

        @pl.when(b >= 2)
        def _():
            wait_sent(psib.at[b % 2], s0_send.at[b % 2])

        slot = ready(g + 1)
        pl.when(b >= 1)(lambda: send1(b - 1))
        at(FOLD1_MID, send2)
        down_quad(1, slot)
        pl.when(b >= 1)(lambda: fold0(b - 1, True))
        combine(psib.at[b % 2], 1 - core)
        start0(b, False)
        combine(pown.at[b], core)
        start0(b, True)
        at(FOLD1_END, fold1)
        return carry

    lax.fori_loop(0, NBW, down_block, 0)

    def ffn_late(i, carry):
        g = G_FFB + 2 * i

        def refill(slot, slot_up):
            pair = i + 4

            @pl.when(pair < N_LATE)
            def _():
                fetch_ffn(slot, FF_EARLY + FF_MID + pair, ffn_gate)
                fetch_ffn(slot_up, FF_EARLY + FF_MID + pair, ffn_up)

            @pl.when(pair >= N_LATE)
            def _():
                fetch_ffn_down(slot, pair - N_LATE, 0)
                fetch_ffn_down(slot_up, pair - N_LATE, 1)

        def before():
            for step, act in ((0, lambda: send2(4)), (1, lambda: send1(NBW - 1)), (2, lambda: send2(5)), (5, lambda: send2(6))):
                pl.when(i == step)(act)

        ffn_pair(g, FF_EARLY + FF_MID + i, refill, before)
        for step, act in ((0, lambda: fold0(NBW - 1, False)), (1, lambda: fold0(NBW - 1, True)), (1, lambda: fold1(5)), (4, lambda: fold1(6))):
            pl.when(i == step)(act)
        return carry

    lax.fori_loop(0, N_LATE, ffn_late, 0)

    def f_copy(n):
        return send(fsend.at[n], frecv.at[n], f_send.at[0], f_recv.at[n], sib)

    def ffn_out(n, carry):
        g = G_FDN + n * N_FK
        held = [ready(g + kk) for kk in range(N_FK)]
        pl.when(n == 2)(lambda: send2(NBW - 1))
        facc[...] = sum(dot(hff[:, kk * DM:(kk + 1) * DM], ring[held[kk]]) for kk in range(N_FK))
        fsend[n] = facc[aligned(1 - core, TOK), :]
        for w in range(CW // BW):
            b = n * (CW // BW) + w
            for half in range(2):
                own = facc[pl.ds(pl.multiple_of(core * TOK + half * HALF, HALF), HALF), w * BW:(w + 1) * BW]
                pown[b, half, 0] = pown[b, half, 0] + own
        pl.when(n >= 1)(lambda: f_copy(n - 1).start())
        pl.when(n == 1)(lambda: fold1(NBW - 1))
        return carry

    lax.fori_loop(0, NCB, ffn_out, 0)

    def final(n):
        f_copy(n).wait_recv()
        for w in range(CW // BW):
            b = n * (CW // BW) + w
            cols = slice(b * BW, (b + 1) * BW)
            wait_got(recv2.at[b], s2_recv.at[b])
            for half in range(2):
                rows = slice(half * HALF, (half + 1) * HALF)
                total = pown[b, half, 0] + recv2[b, half] + frecv[n, rows, w * BW:(w + 1) * BW]
                out[rows, cols] = (a_s[rows, cols].astype(F32) + total).astype(BF16)

    final(0)
    f_copy(NCB - 1).start()
    final(1)
    final(2)
    wait_sent(pown.at[pl.ds(0, 4)], s1_send.at[0])
    for parity in range(2):
        wait_sent(psib.at[parity], s0_send.at[parity])
    wait_sent(fsend, f_send.at[0])
    final(3)
    wait_sent(pown.at[pl.ds(0, 2)], s2_send.at[0])


def rope_tables():
    half = HEAD // 2
    inv_freq = np.float32(ROPE_BASE) ** (np.float32(-2.0) * np.arange(half, dtype=np.float32) / np.float32(HEAD))
    angles = np.arange(TOK, dtype=np.float32)[:, None] * inv_freq[None, :].astype(np.float32)
    cos_h, sin_h = np.cos(angles).astype(np.float32), np.sin(angles).astype(np.float32)
    return np.concatenate([cos_h, cos_h], axis=1), np.concatenate([-sin_h, sin_h], axis=1)


def solution(mesh):
    row_spec = P(('dp', 'ep'), None, None)
    vec_spec = P(None)
    mat_spec = P(None, None)
    cube_spec = P(None, None, None)
    expert_spec = P('ep', None, None)
    vmem = pl.BlockSpec(memory_space=pltpu.VMEM)
    hbm = pl.BlockSpec(memory_space=pl.ANY)

    def per_device(hidden, expert_ids, slot_ids, attn_norm, w_query, w_key, w_value, w_out, ffn_norm, ffn_gate, ffn_up, ffn_down, moe_norm, w_router, exp_gate, exp_up, exp_down):
        cos_t, sin_t = rope_tables()
        dma = pltpu.SemaphoreType.DMA
        call = pl.pallas_call(
            kernel,
            out_shape=pltpu.VMEM((TOK, DM), BF16),
            in_specs=[hbm] * 19,
            out_specs=vmem,
            scratch_shapes=[
                pltpu.VMEM((NSLOT, DM, CW), BF16),
                pltpu.VMEM((DEVS, NCB * TOK, CW), BF16),
                pltpu.VMEM((LOCAL, DEVS * CAP, DM), BF16),
                pltpu.VMEM((LOCAL, DEVS * CAP, EFF), BF16),
                pltpu.VMEM((NBW, 2, 4, HALF, BW), F32),
                pltpu.VMEM((2, 2, 4, HALF, BW), F32),
                pltpu.VMEM((4, 2, 4, HALF, BW), F32),
                pltpu.VMEM((NBW, 2, 2, HALF, BW), F32),
                pltpu.VMEM((NBW, 2, HALF, BW), F32),
                pltpu.VMEM((DEVS, 3 * TOK, ROWS), BF16),
                pltpu.VMEM((ROWS, TOK), BF16),
                pltpu.VMEM((DEVS, 2 * TOPK, TOK), F32),
                pltpu.VMEM((TOK, DM), BF16),
                pltpu.VMEM((2 * TOK, DM), BF16),
                pltpu.VMEM((NCB, TOK, CW), F32),
                pltpu.VMEM((NCB, TOK, CW), F32),
                pltpu.VMEM((TOK, DM), BF16),
                pltpu.VMEM((2 * TOK, FF // 2), BF16),
                pltpu.VMEM((2 * TOK, CW), F32),
                pltpu.VMEM((2, TOK, CW), BF16),
                pltpu.VMEM((2, TOK, CW), BF16),
                pltpu.VMEM((2, TOK, CW), BF16),
                dma((NSLOT,)), dma((1,)), dma((12,)), dma((1,)), dma((1,)),
                dma((2,)), dma((NBW, 2)), dma((1,)), dma((NBW,)), dma((1,)), dma((NBW,)),
                dma(()), dma(()), dma((1,)), dma((NCB,)), dma((9,)),
                pltpu.VMEM((TOK, DM), BF16),
                pltpu.VMEM((TOPK, TOK), jnp.int32),
                pltpu.VMEM((TOPK, TOK), jnp.int32),
                pltpu.VMEM((DM // LANE, LANE), BF16),
                pltpu.VMEM((DM // LANE, LANE), BF16),
                pltpu.VMEM((DM // LANE, LANE), BF16),
                pltpu.VMEM((NEXP, DM), BF16),
                pltpu.VMEM((TOK, HEAD), F32),
                pltpu.VMEM((TOK, HEAD), F32),
            ],
            compiler_params=pltpu.CompilerParams(collective_id=0, has_side_effects=True, vmem_limit_bytes=66000000),
            cost_estimate=pl.CostEstimate(flops=56_000_000_000, bytes_accessed=240_000_000, transcendentals=0),
        )
        res = call(
            hidden.reshape(TOK, DM), expert_ids.reshape(TOK, TOPK).T, slot_ids.reshape(TOK, TOPK).T,
            attn_norm.reshape(DM // LANE, LANE), ffn_norm.reshape(DM // LANE, LANE), moe_norm.reshape(DM // LANE, LANE), w_router.T, cos_t, sin_t,
            w_query, w_key, w_value, w_out.reshape(DM, DM), ffn_gate, ffn_up, ffn_down, exp_gate, exp_up, exp_down)
        return res.reshape(hidden.shape)

    return jax.shard_map(per_device, mesh=mesh, in_specs=(row_spec, row_spec, row_spec, vec_spec, mat_spec, mat_spec, mat_spec, cube_spec, vec_spec, mat_spec, mat_spec, mat_spec, vec_spec, mat_spec, expert_spec, expert_spec, expert_spec), out_specs=row_spec, check_vma=False)
```
